256 devices in a mesh: section: 4 (over y_lo, core), expert: 64 (over y_hi, x, z).
Axes of the slice: x: 4, y: 4 (y_hi: 2, y_lo: 2; y = y_hi * 2 + y_lo), z: 8, core: 2. Of those that a mesh axis runs over, the one named last changes fastest.
Arguments:
- activations: bfloat16 [4, 2048, 4096], P('section', 'expert'), may hold values from -6 to 6
- norm_gain: float32 [4, 4096], P('section'), may hold values from 0.25 to 1.75
- in_proj: bfloat16 [4, 4096, 40960], P('section', None, 'expert'), may hold values from -0.09375 to 0.09375
- out_proj: bfloat16 [4, 40960, 4096], P('section', 'expert'), may hold values from -0.078125 to 0.078125
- expert_ids: int32 [4, 2048, 1], P('section', 'expert'), may hold values from 0 to 7; in each aligned block of 32 rows (0 to 31, 32 to 63, ..., all dimensions but the last counted through in order) at most 8 rows name the same one
Outputs:
- passed: bfloat16 [4, 2048, 4096], P('section', 'expert')
The draws below stay inside these ranges and needn't reach their ends.
Inputs may be any that keep to these rules, and one draw needn't show every extreme that they name: `expert_ids`: within the 32 rows of one device (aligned blocks of 32 rows along the token dimension of each layer), no expert is named by more than 8 rows.
All inputs are finite; a program needn't handle non-finite values.
Results may differ from the reference program's by a relative error of at most 0.0047.
Values may be sent and summed in bfloat16 or wider, within the bound.
A program may use at most 64 MiB of HBM per device.

```python
import math
import jax
import jax.numpy as jnp
import numpy as np
from jax import lax

D = 4096
FF_W = 5120
EXPERTS = 8
MB_TOK = 32
CAP = 8
TOKENS = 2048
N_SECTION = 4
N_EXPERT = 64


def steps_of(stream_key, dims, split, smallest, largest):
    gain, own = 1.0, jax.random.fold_in(stream_key, 6)
    for dim, parts in split:
        steps = jnp.exp(jax.random.uniform(jax.random.fold_in(own, dim), (parts,), jnp.float32, smallest / len(split), largest / len(split)))
        gain = gain * jnp.repeat(steps, dims[dim] // parts).reshape([-1 if axis == dim else 1 for axis in range(len(dims))])
    return gain


def shared_out(own_key, own, number, rows, number_of, top, bound, lean):
    order = jax.random.permutation(own_key, number_of)
    heavy_load, common = portions_of(number_of, rows * top, bound, lean, True), portions_of(number_of, rows * top, bound, lean, False)
    places = jnp.arange(number_of)

    def named(lengths, turn):
        used = int((lengths > 0).sum())
        fixed = max(1, used // 4)
        shifted = fixed + (places - fixed + turn * (used - fixed)) % max(1, number_of - fixed)
        return jnp.zeros((number_of,), jnp.int32).at[order[jnp.where(places < fixed, places, shifted)]].set(jnp.asarray(lengths, jnp.int32))

    lengths = jnp.where(number % 4 == 0, named(heavy_load, number // 4), named(common, number - number // 4 - 1))
    mixed = jax.random.permutation(jax.random.fold_in(own, 3), number_of)
    source_of, sink = mixed[0:number_of // 2 * 2:2], mixed[1:number_of // 2 * 2:2]
    margin = jnp.minimum(lengths[source_of] - 1, bound - lengths[sink]) // 2
    margin = jnp.where((source_of == order[0]) | (sink == order[0]) | (lengths[sink] == 0), 0, jnp.maximum(margin, 0))
    shifted = jax.random.randint(jax.random.fold_in(own, 4), (number_of // 2,), 0, 1 << 20) % (margin + 1)
    lengths = lengths.at[source_of].add(-shifted).at[sink].add(shifted)
    members = jnp.searchsorted(jnp.cumsum(lengths), jnp.arange(rows * top), side="right").astype(jnp.int32)
    listing = members.reshape(top, rows).T
    listing = listing[jax.random.permutation(jax.random.fold_in(own, 1), rows)]
    turn = jax.random.randint(jax.random.fold_in(own, 2), (rows, 1), 0, top)
    return jnp.take_along_axis(listing, (jnp.arange(top)[None, :] + turn) % top, axis=1)


def portions_of(count, total, most, slope, full):
    portions = [(1 << 20) // math.isqrt(grade ** slope) + 1 for grade in range(1, count + 1)]
    largest = most if full else min(most, max(-(-total // count), total * portions[0] // sum(portions)))
    least = 1 if total - largest >= count - 1 else 0
    given, spare = [largest] + [least] * (count - 1), total - largest - least * (count - 1)
    while spare > 0:
        candidates = [i for i in range(1, count) if given[i] < largest] or [i for i in range(1, count) if given[i] < most]
        mass, remaining = sum([portions[i] for i in candidates]), spare
        for i in candidates:
            extra = min(most - given[i], max(1, remaining * portions[i] // mass), spare)
            given[i] = given[i] + extra
            spare = spare - extra
    return np.array(given)


def centred(key, shape, width, most, shards=(), kind=jnp.bfloat16):
    factor_of = steps_of(key, shape, shards, -0.22, 0.18) if shards else 1.0
    drawn = jax.random.normal(key, shape, jnp.float32) * width * factor_of
    return jnp.minimum(jnp.maximum(drawn, -most), most).astype(kind)


def setup_inputs(seed: int = 0) -> dict:
    key_list = jax.random.split(jax.random.key(seed), 6)
    activations = centred(key_list[0], (N_SECTION, TOKENS, D), 1.0, 6.0, ((0, 4), (1, 64)))
    norm_gain = jnp.clip(1.0 + 0.15 * jax.random.normal(key_list[1], (N_SECTION, D), jnp.float32), 0.25, 1.75)
    in_proj = centred(key_list[2], (N_SECTION, D, EXPERTS * FF_W), D ** -0.5, 0.09375, ((0, 4), (2, 64)))
    out_proj = centred(key_list[3], (N_SECTION, EXPERTS * FF_W, D), FF_W ** -0.5, 0.078125, ((0, 4), (1, 64)))
    expert_ids_keys = jax.random.split(jax.random.fold_in(key_list[4], 1), N_SECTION * TOKENS // MB_TOK)
    expert_ids_turns = jax.random.permutation(jax.random.fold_in(key_list[4], 3), N_SECTION * TOKENS // MB_TOK)
    expert_ids = jax.vmap(lambda own, number: shared_out(jax.random.fold_in(key_list[4], 2), own, number, MB_TOK, EXPERTS, 1, CAP, 2))(expert_ids_keys, expert_ids_turns).reshape((N_SECTION, TOKENS, 1))
    return {"activations": activations, "norm_gain": norm_gain, "in_proj": in_proj, "out_proj": out_proj, "expert_ids": expert_ids}


epsilon = 1e-06

def reference(activations, norm_gain, in_proj, out_proj, expert_ids):
    groups = N_EXPERT // EXPERTS
    slice_width = FF_W // groups
    results = []
    for section_index in range(N_SECTION):
        floats = activations[section_index].astype(jnp.float32)
        scale = lax.rsqrt(lax.optimization_barrier(jnp.mean(floats * floats, axis=-1, keepdims=True)) + epsilon)
        normed = (floats * scale * norm_gain[section_index][None, :]).astype(jnp.bfloat16)
        routed = expert_ids[section_index, :, 0].astype(jnp.int32)
        onehot = (routed[:, None] == jnp.arange(EXPERTS, dtype=jnp.int32)[None, :]).astype(jnp.int32)
        blocked = onehot.reshape(N_EXPERT, MB_TOK, EXPERTS)
        before = (jnp.cumsum(blocked, axis=1) - blocked).reshape(TOKENS, EXPERTS)
        ranks = lax.optimization_barrier(jnp.sum(before * onehot, axis=1)).astype(jnp.int32)
        slots = (jnp.arange(TOKENS, dtype=jnp.int32) // MB_TOK * CAP + ranks).astype(jnp.int32)
        buffer = jnp.zeros((EXPERTS, N_EXPERT * CAP, D), jnp.bfloat16).at[routed, slots].set(normed)
        first_proj = in_proj[section_index].reshape(D, EXPERTS, FF_W).transpose(1, 0, 2)
        second_proj = out_proj[section_index].reshape(EXPERTS, FF_W, D)

        def expert(operands):
            inputs, first, second = operands
            preact = jnp.dot(inputs, first, preferred_element_type=jnp.float32)
            hidden = jax.nn.gelu(preact, approximate=True).astype(jnp.bfloat16)
            summed = jnp.zeros((inputs.shape[0], D), jnp.float32)
            for shard in range(groups):
                piece = jnp.dot(hidden[:, shard * slice_width:(shard + 1) * slice_width], second[shard * slice_width:(shard + 1) * slice_width], preferred_element_type=jnp.float32)
                summed = summed + piece
            return summed
        outputs = lax.map(expert, (buffer, first_proj, second_proj))
        mixed_rows = outputs[routed, slots]
        results.append((floats + mixed_rows).astype(jnp.bfloat16))
    return jnp.roll(jnp.stack(results), 1, axis=0)
```

```python
import functools

import jax
import jax.numpy as jnp
from jax import lax
from jax.experimental import pallas as pl
from jax.experimental.pallas import tpu as pltpu
from jax.sharding import PartitionSpec as P

EXPERTS = 8
RING = 8
NX = 4
NEAR = ((0, 0), (0, 1), (0, 3), (1, 0), (0, 2), (1, 1), (1, 3), (1, 2))
MESH = pl.DeviceIdType.MESH
F32, BF16 = jnp.float32, jnp.bfloat16

epsilon = 1e-06


def neighbour(group, o):
    dy, dx = NEAR[o]
    return lax.rem(group // NX + dy, EXPERTS // NX) * NX + lax.rem(group % NX + dx, NX)


def mirrored(o):
    dy, dx = NEAR[o]
    return NEAR.index((dy, (NX - dx) % NX))


def placement(routed, ranks, capacity, group, rows):
    row = lax.broadcasted_iota(jnp.int32, (rows, routed.shape[1]), 0)
    place = row // capacity
    owner = jnp.full_like(place, -1)
    for o in range(EXPERTS):
        owner = jnp.where(place == o, neighbour(group, o), owner)
    return jnp.where((owner == routed) & (row % capacity == ranks), 1.0, 0.0).astype(F32)


def arrived(ref, sem):
    pltpu.make_async_copy(ref, ref, sem).wait()


def kernel(
    sections, n, capacity, act_hbm, gain_hbm, ids_hbm, first_hbm, second_hbm, out,
    act, gain, ids, first, second, normed, packed, gathered, hidden, partial, sending, arriving, summed, returned,
    where_to, residual, where_from,
    small_sem, weight_sem, pass_send, pass_recv, give_send, ring_send, ring_recv, sum_recv, back_send, back_recv,
):
    section, me = lax.axis_index("section"), lax.axis_index("expert")
    following, leading = lax.rem(section + 1, sections), lax.rem(section + sections - 1, sections)
    group, z = me // RING, lax.rem(me, RING)
    tokens, width = act.shape
    ff = hidden.shape[1]
    rows = EXPERTS * capacity

    def along(k):
        return lax.rem(z + k, RING)

    def on_ring(k):
        return (section, group * RING + along(k))

    def in_plane(o, which):
        return (which, neighbour(group, o) * RING + z)

    smalls = [
        pltpu.make_async_copy(act_hbm.at[0], act, small_sem.at[0]),
        pltpu.make_async_copy(gain_hbm, gain, small_sem.at[1]),
        pltpu.make_async_copy(ids_hbm, ids, small_sem.at[2]),
    ]
    weights = [
        pltpu.make_async_copy(first_hbm.at[0], first, weight_sem.at[0]),
        pltpu.make_async_copy(second_hbm.at[0], second, weight_sem.at[1]),
    ]
    for copy in smalls:
        copy.start()
    barrier = pltpu.get_barrier_semaphore()
    greeted = [in_plane(o, section) for o in range(1, EXPERTS)] + [on_ring(1), on_ring(RING - 1)]
    greeted += [in_plane(o, leading) for o in range(EXPERTS)]
    for peer in greeted:
        pl.semaphore_signal(barrier, inc=1, device_id=peer, device_id_type=MESH)
    for copy in smalls:
        copy.wait()
    for copy in weights:
        copy.start()

    floats = act[...].astype(F32)
    scale = lax.rsqrt(jnp.mean(floats * floats, axis=-1, keepdims=True) + epsilon)
    normed[...] = (floats * scale * gain[...]).astype(BF16)
    routed = ids[...]
    expert = lax.broadcasted_iota(jnp.int32, (EXPERTS, tokens), 0)
    onehot = jnp.where(expert == routed, 1.0, 0.0).astype(F32)
    earlier = lax.broadcasted_iota(jnp.int32, (tokens, tokens), 0) < lax.broadcasted_iota(
        jnp.int32, (tokens, tokens), 1
    )
    before = jnp.dot(
        onehot.astype(BF16), jnp.where(earlier, 1.0, 0.0).astype(BF16), preferred_element_type=F32
    )
    ranks = jnp.sum(before * onehot, axis=0, keepdims=True).astype(jnp.int32)
    placing = placement(routed, ranks, capacity, group, where_to.shape[1])
    where_to[...] = placing.T.astype(BF16)
    placing = placing[:rows].astype(BF16)
    step = 512
    for c in range(width // step):
        cols = slice(c * step, (c + 1) * step)
        block = jnp.dot(placing, normed[:, cols], preferred_element_type=F32)
        packed[:, :, cols] = block.astype(BF16).reshape(EXPERTS, capacity, step)
    gathered[z, 0] = packed[0]

    pl.semaphore_wait(barrier, len(greeted))

    def forward(block, o, k, way):
        pltpu.make_async_remote_copy(
            src_ref=gathered.at[block, o], dst_ref=gathered.at[block, o],
            send_sem=ring_send.at[way], recv_sem=ring_recv.at[block, o],
            device_id=on_ring(k), device_id_type=MESH,
        ).start()

    forward(z, 0, 1, 0)
    forward(z, 0, RING - 1, 1)
    for o in range(1, EXPERTS):
        pltpu.make_async_remote_copy(
            src_ref=packed.at[o], dst_ref=gathered.at[z, mirrored(o)],
            send_sem=give_send.at[0], recv_sem=ring_recv.at[z, mirrored(o)],
            device_id=in_plane(o, section), device_id_type=MESH,
        ).start()
    passes = [
        pltpu.make_async_remote_copy(
            src_ref=src, dst_ref=dst, send_sem=pass_send.at[k], recv_sem=pass_recv.at[k],
            device_id=(following, me), device_id_type=MESH,
        )
        for k, (src, dst) in enumerate(((act, residual), (where_to, where_from)))
    ]
    for copy in passes:
        copy.start()

    def spread(o, carry):
        arrived(gathered.at[z, o], ring_recv.at[z, o])
        forward(z, o, 1, 0)
        forward(z, o, RING - 1, 1)
        return carry

    lax.fori_loop(1, EXPERTS, spread, 0)
    for copy in weights:
        copy.wait()

    def pass_on(way, j, o, add):
        distance = RING // 2 - j
        block = along(distance if way == 0 else RING - distance)
        value = partial[block, o]
        if add:
            arrived(arriving.at[way, j - 1, o], sum_recv.at[way, j - 1, o])
            value = value + arriving[way, j - 1, o].astype(F32)
        sending[way, j, o] = value.astype(BF16)
        pltpu.make_async_remote_copy(
            src_ref=sending.at[way, j, o], dst_ref=arriving.at[way, j, o],
            send_sem=ring_send.at[way], recv_sem=sum_recv.at[way, j, o],
            device_id=on_ring(1 if way == 0 else RING - 1), device_id_type=MESH,
        ).start()

    half = RING // 2

    def gather(k, carry):
        left, right = along(RING - k), along(k)

        def hop(o, inner):
            arrived(gathered.at[left, o], ring_recv.at[left, o])

            @pl.when((k < half - 1) | ((k == half - 1) & (o % 2 == 0)))
            def _():
                forward(left, o, 1, 0)

            @pl.when(k < half)
            def _():
                arrived(gathered.at[right, o], ring_recv.at[right, o])

            @pl.when((k < half - 1) | ((k == half - 1) & (o % 2 == 1)))
            def _():
                forward(right, o, RING - 1, 1)

            return inner

        lax.fori_loop(0, EXPERTS, hop, 0)
        other = jnp.where(k < half, right, z)
        inputs = jnp.concatenate(
            [gathered[left].reshape(rows, width), gathered[other].reshape(rows, width)], axis=0
        )
        value = jnp.dot(inputs, first[...], preferred_element_type=F32)
        hidden[...] = jax.nn.gelu(value, approximate=True).astype(BF16)

        def tile(t, inner):
            cols = pl.ds(pl.multiple_of(t * step, step), step)
            piece = jnp.dot(hidden[...], second[:, cols], preferred_element_type=F32)
            piece = piece.reshape(2, EXPERTS, capacity, step)
            partial[left, :, :, cols] = piece[0]
            partial[other, :, :, cols] = piece[1]
            return inner

        lax.fori_loop(0, width // step, tile, 0)

        @pl.when(k == half - 1)
        def _():
            def early(i, inner):
                pass_on(0, 1, EXPERTS - 1 - 2 * i, False)
                pass_on(1, 1, EXPERTS - 2 - 2 * i, False)
                return inner

            lax.fori_loop(0, EXPERTS // 2, early, 0)

        return carry

    lax.fori_loop(1, half + 1, gather, 0)

    def start(i, carry):
        pass_on(0, 0, EXPERTS - 2 - 2 * i, False)
        pass_on(1, 0, EXPERTS - 1 - 2 * i, False)
        return carry

    lax.fori_loop(0, EXPERTS // 2, start, 0)

    def second_hop(i, carry):
        pass_on(0, 1, EXPERTS - 2 - 2 * i, True)
        pass_on(1, 1, EXPERTS - 1 - 2 * i, True)
        return carry

    lax.fori_loop(0, EXPERTS // 2, second_hop, 0)
    for j in range(2, half):
        def later(i, carry):
            pass_on(0, j, EXPERTS - 1 - i, True)
            pass_on(1, j, EXPERTS - 1 - i, True)
            return carry

        lax.fori_loop(0, EXPERTS, later, 0)

    for o in reversed(range(EXPERTS)):
        value = partial[z, o]
        for way in range(2):
            arrived(arriving.at[way, half - 1, o], sum_recv.at[way, half - 1, o])
            value = value + arriving[way, half - 1, o].astype(F32)
        summed[o] = value.astype(BF16)
        pltpu.make_async_remote_copy(
            src_ref=summed.at[o], dst_ref=returned.at[mirrored(o)],
            send_sem=back_send.at[0], recv_sem=back_recv.at[mirrored(o)],
            device_id=in_plane(o, following), device_id_type=MESH,
        ).start()

    for copy in passes:
        copy.wait()
    for o in reversed(range(EXPERTS)):
        arrived(returned.at[o], back_recv.at[o])
    picks = where_from[:, :rows]
    for c in range(width // step):
        cols = slice(c * step, (c + 1) * step)
        mixed = jnp.dot(picks, returned[:, :, cols].reshape(rows, step), preferred_element_type=F32)
        out[0, :, cols] = (residual[:, cols].astype(F32) + mixed).astype(BF16)

    arrived(packed.at[pl.ds(1, EXPERTS - 1)], give_send.at[0])
    for way in range(2):
        arrived(gathered.at[pl.ds(0, RING - 1)], ring_send.at[way])
    arrived(summed, back_send.at[0])


def per_device(sections, n, activations, norm_gain, in_proj, out_proj, expert_ids):
    tokens, width = activations.shape[1:]
    ff = in_proj.shape[2]
    capacity = 2 * tokens // EXPERTS
    rows = EXPERTS * capacity
    dma = pltpu.SemaphoreType.DMA
    half = RING // 2
    return pl.pallas_call(
        functools.partial(kernel, sections, n, capacity),
        out_shape=pltpu.VMEM(activations.shape, activations.dtype),
        in_specs=[pl.BlockSpec(memory_space=pl.ANY)] * 5,
        out_specs=pl.BlockSpec(memory_space=pltpu.VMEM),
        scratch_shapes=[
            pltpu.VMEM((tokens, width), BF16),
            pltpu.VMEM((1, width), F32),
            pltpu.VMEM((1, tokens), jnp.int32),
            pltpu.VMEM((width, ff), BF16),
            pltpu.VMEM((ff, width), BF16),
            pltpu.VMEM((tokens, width), BF16),
            pltpu.VMEM((EXPERTS, capacity, width), BF16),
            pltpu.VMEM((RING, EXPERTS, capacity, width), BF16),
            pltpu.VMEM((2 * rows, ff), BF16),
            pltpu.VMEM((RING, EXPERTS, capacity, width), F32),
            pltpu.VMEM((2, half, EXPERTS, capacity, width), BF16),
            pltpu.VMEM((2, half, EXPERTS, capacity, width), BF16),
            pltpu.VMEM((EXPERTS, capacity, width), BF16),
            pltpu.VMEM((EXPERTS, capacity, width), BF16),
            pltpu.VMEM((tokens, 128), BF16),
            pltpu.VMEM((tokens, width), BF16),
            pltpu.VMEM((tokens, 128), BF16),
            dma((3,)),
            dma((2,)),
            dma((2,)),
            dma((2,)),
            dma((1,)),
            dma((2,)),
            dma((RING, EXPERTS)),
            dma((2, half, EXPERTS)),
            dma((1,)),
            dma((EXPERTS,)),
        ],
        compiler_params=pltpu.CompilerParams(
            collective_id=0, has_side_effects=True, vmem_limit_bytes=62 * 1024 * 1024
        ),
    )(activations, norm_gain, expert_ids.reshape(1, tokens), in_proj, out_proj)


def solution(mesh):
    return jax.shard_map(
        functools.partial(per_device, mesh.shape["section"], mesh.shape["expert"]),
        mesh=mesh,
        in_specs=(
            P("section", "expert", None),
            P("section", None),
            P("section", None, "expert"),
            P("section", "expert", None),
            P("section", "expert", None),
        ),
        out_specs=P("section", "expert", None),
        check_vma=False,
    )
```

```python
import functools

import jax
import jax.numpy as jnp
from jax import lax
from jax.experimental import pallas as pl
from jax.experimental.pallas import tpu as pltpu
from jax.sharding import PartitionSpec as P

EXPERTS = 8
RING = 8
NX = 4
FLAT = 2048
PIECES = 4
LANES = 128
STEP = 512
NEAR = ((0, 0), (0, 1), (0, 3), (1, 0), (0, 2), (1, 1), (1, 3), (1, 2))
MESH = pl.DeviceIdType.MESH
F32, BF16 = jnp.float32, jnp.bfloat16

epsilon = 1e-06


def neighbour(group, o):
    dy, dx = NEAR[o]
    return lax.rem(group // NX + dy, EXPERTS // NX) * NX + lax.rem(group % NX + dx, NX)


def mirrored(o):
    dy, dx = NEAR[o]
    return NEAR.index((dy, (NX - dx) % NX))


def placement(routed, ranks, capacity, group, rows):
    row = lax.broadcasted_iota(jnp.int32, (rows, routed.shape[1]), 0)
    place = row // capacity
    owner = jnp.full_like(place, -1)
    for o in range(EXPERTS):
        owner = jnp.where(place == o, neighbour(group, o), owner)
    return jnp.where((owner == routed) & (row % capacity == ranks), 1.0, 0.0).astype(F32)


def arrived(ref, sem):
    pltpu.make_async_copy(ref, ref, sem).wait()


def kernel(
    sections, n, capacity, act_hbm, gain_hbm, ids_hbm, first_hbm, second_hbm, out,
    act, gain, ids, first, second, normed, packed, slots, flat, spread_out, spread_in, hidden,
    partial, sending, arriving, summed, returned,
    parts_out, parts_in, whole, flat_sending, flat_arriving, flat_summed, flat_returned,
    where_to, residual, where_from,
    small_sem, weight_sem, pass_send, pass_recv, give_send, ring_send, ring_recv, sum_recv, back_send, back_recv,
    flat_send, flat_recv, plane_send, plane_recv, parts_send, parts_recv, flat_sum_send, flat_sum_recv,
    flat_back_send, flat_back_recv,
):
    section, me = lax.axis_index("section"), lax.axis_index("expert")
    following, leading = lax.rem(section + 1, sections), lax.rem(section + sections - 1, sections)
    group, z = me // RING, lax.rem(me, RING)
    tokens, width = act.shape
    rows = EXPERTS * capacity
    rest = width - FLAT
    half = RING // 2
    piece = tokens // PIECES
    last = RING - 1

    def along(k):
        return lax.rem(z + k, RING)

    def on_ring(k):
        return (section, group * RING + along(k))

    def in_plane(o, which):
        return (which, neighbour(group, o) * RING + z)

    smalls = [
        pltpu.make_async_copy(act_hbm.at[0], act, small_sem.at[0]),
        pltpu.make_async_copy(gain_hbm, gain, small_sem.at[1]),
        pltpu.make_async_copy(ids_hbm, ids, small_sem.at[2]),
    ]
    weights = [
        pltpu.make_async_copy(first_hbm.at[0], first, weight_sem.at[0]),
        pltpu.make_async_copy(second_hbm.at[0], second, weight_sem.at[1]),
    ]
    for copy in smalls:
        copy.start()
    barrier = pltpu.get_barrier_semaphore()
    greeted = [in_plane(o, section) for o in range(1, EXPERTS)] + [on_ring(1), on_ring(last)]
    greeted += [in_plane(o, leading) for o in range(EXPERTS)]
    for peer in greeted:
        pl.semaphore_signal(barrier, inc=1, device_id=peer, device_id_type=MESH)
    for copy in smalls:
        copy.wait()
    for copy in weights:
        copy.start()

    floats = act[...].astype(F32)
    scale = lax.rsqrt(jnp.mean(floats * floats, axis=-1, keepdims=True) + epsilon)
    values = (floats * scale * gain[...]).astype(BF16)
    normed[...] = values[:, FLAT:]
    flat[z, :, :, :FLAT] = values[:, :FLAT].reshape(PIECES, piece, FLAT)
    routed = ids[...]
    expert = lax.broadcasted_iota(jnp.int32, (EXPERTS, tokens), 0)
    onehot = jnp.where(expert == routed, 1.0, 0.0).astype(F32)
    earlier = lax.broadcasted_iota(jnp.int32, (tokens, tokens), 0) < lax.broadcasted_iota(
        jnp.int32, (tokens, tokens), 1
    )
    before = jnp.dot(
        onehot.astype(BF16), jnp.where(earlier, 1.0, 0.0).astype(BF16), preferred_element_type=F32
    )
    ranks = jnp.sum(before * onehot, axis=0, keepdims=True).astype(jnp.int32)
    placing = placement(routed, ranks, capacity, group, LANES)
    back = placing.T.astype(BF16)
    where_to[...] = back
    flat[z, :, :, FLAT:] = back.reshape(PIECES, piece, LANES)
    placing = placing[:rows].astype(BF16)

    pl.semaphore_wait(barrier, len(greeted))

    def forward_flat(block, c, k):
        pltpu.make_async_remote_copy(
            src_ref=flat.at[block, c], dst_ref=flat.at[block, c],
            send_sem=flat_send.at[0], recv_sem=flat_recv.at[block, c],
            device_id=on_ring(k), device_id_type=MESH,
        ).start()

    def forward(block, o, k, way):
        pltpu.make_async_remote_copy(
            src_ref=slots.at[block, o], dst_ref=slots.at[block, o],
            send_sem=ring_send.at[way], recv_sem=ring_recv.at[block, o],
            device_id=on_ring(k), device_id_type=MESH,
        ).start()

    for c in range(PIECES):
        forward_flat(z, c, 1)
        forward_flat(z, c, last)

    for c in range(rest // STEP):
        cols = slice(c * STEP, (c + 1) * STEP)
        block = jnp.dot(placing, normed[:, cols], preferred_element_type=F32)
        packed[:, :, cols] = block.astype(BF16).reshape(EXPERTS, capacity, STEP)
    slots[z, 0] = packed[0]
    for o in range(1, EXPERTS):
        pltpu.make_async_remote_copy(
            src_ref=packed.at[o], dst_ref=slots.at[z, mirrored(o)],
            send_sem=give_send.at[0], recv_sem=ring_recv.at[z, mirrored(o)],
            device_id=in_plane(o, section), device_id_type=MESH,
        ).start()
    forward(z, 0, 1, 0)
    forward(z, 0, last, 1)

    def routes(block):
        return flat[block, :, :, FLAT:].reshape(tokens, LANES)

    def pack(block):
        to_slot = routes(block).astype(F32).T[:rows].astype(BF16)
        for c in range(FLAT // STEP):
            cols = slice(c * STEP, (c + 1) * STEP)
            source = flat[block, :, :, cols].reshape(tokens, STEP)
            value = jnp.dot(to_slot, source, preferred_element_type=F32)
            value = value.astype(BF16).reshape(EXPERTS, capacity, STEP)
            spread_out[block, :, :, cols] = value
            spread_in[block, 0, :, cols] = value[0]
        for o in range(1, EXPERTS):
            pltpu.make_async_remote_copy(
                src_ref=spread_out.at[block, o], dst_ref=spread_in.at[block, mirrored(o)],
                send_sem=plane_send.at[0], recv_sem=plane_recv.at[block],
                device_id=in_plane(o, section), device_id_type=MESH,
            ).start()

    pack(z)
    passes = [
        pltpu.make_async_remote_copy(
            src_ref=src, dst_ref=dst, send_sem=pass_send.at[k], recv_sem=pass_recv.at[k],
            device_id=(following, me), device_id_type=MESH,
        )
        for k, (src, dst) in enumerate(((act.at[:, pl.ds(FLAT, rest)], residual), (where_to, where_from)))
    ]
    for copy in passes:
        copy.start()

    def ring_flat(k):
        left, right = along(RING - k), along(k)

        def hop(c, inner):
            arrived(flat.at[left, c], flat_recv.at[left, c])
            if k < half - 1:
                forward_flat(left, c, 1)
            if k < half:
                arrived(flat.at[right, c], flat_recv.at[right, c])
            if k < half - 1:
                forward_flat(right, c, last)
            if k == half - 1:
                @pl.when(c % 2 == 0)
                def _():
                    forward_flat(left, c, 1)

                @pl.when(c % 2 == 1)
                def _():
                    forward_flat(right, c, last)

            return inner

        lax.fori_loop(0, PIECES, hop, 0)

        def fill(i, inner):
            pack(along(jnp.where(i == 0, RING - k, k)))
            return inner

        lax.fori_loop(0, 2 if k < half else 1, fill, 0)

    def spread(o, carry):
        arrived(slots.at[z, o], ring_recv.at[z, o])
        forward(z, o, 1, 0)
        forward(z, o, last, 1)
        return carry

    def ring_slots(k, low, high):
        left, right = along(RING - k), along(k)

        def hop(o, inner):
            arrived(slots.at[left, o], ring_recv.at[left, o])

            @pl.when((k < half - 1) | ((k == half - 1) & (o % 2 == 0)))
            def _():
                forward(left, o, 1, 0)

            @pl.when(k < half)
            def _():
                arrived(slots.at[right, o], ring_recv.at[right, o])

            @pl.when((k < half - 1) | ((k == half - 1) & (o % 2 == 1)))
            def _():
                forward(right, o, last, 1)

            return inner

        lax.fori_loop(low, high, hop, 0)

    ring_flat(1)
    lax.fori_loop(1, EXPERTS // 2, spread, 0)
    ring_flat(2)
    lax.fori_loop(EXPERTS // 2, EXPERTS, spread, 0)
    ring_flat(3)
    ring_slots(jnp.int32(1), 0, EXPERTS // 2)
    ring_flat(4)
    ring_slots(jnp.int32(1), EXPERTS // 2, EXPERTS)
    for copy in weights:
        copy.wait()

    def pass_on(way, j, o, add):
        distance = half - j
        block = along(distance if way == 0 else RING - distance)
        value = partial[block, o]
        if add:
            arrived(arriving.at[way, j - 1, o], sum_recv.at[way, j - 1, o])
            value = value + arriving[way, j - 1, o].astype(F32)
        sending[way, j, o] = value.astype(BF16)
        pltpu.make_async_remote_copy(
            src_ref=sending.at[way, j, o], dst_ref=arriving.at[way, j, o],
            send_sem=ring_send.at[way], recv_sem=sum_recv.at[way, j, o],
            device_id=on_ring(1 if way == 0 else last), device_id_type=MESH,
        ).start()

    def pass_flat(way, j, c, add):
        distance = half - j
        block = along(distance if way == 0 else RING - distance)
        value = whole[block, c]
        if add:
            arrived(flat_arriving.at[way, j - 1, c], flat_sum_recv.at[way, j - 1, c])
            value = value + flat_arriving[way, j - 1, c].astype(F32)
        place = (way * half + j) * PIECES + c
        flat_sending[place] = value.astype(BF16)
        pltpu.make_async_remote_copy(
            src_ref=flat_sending.at[place], dst_ref=flat_arriving.at[way, j, c],
            send_sem=flat_sum_send.at[0], recv_sem=flat_sum_recv.at[way, j, c],
            device_id=on_ring(1 if way == 0 else last), device_id_type=MESH,
        ).start()

    def give_back(block):
        for o in range(1, EXPERTS):
            pltpu.make_async_remote_copy(
                src_ref=parts_out.at[block, o], dst_ref=parts_in.at[block, mirrored(o)],
                send_sem=parts_send.at[0], recv_sem=parts_recv.at[block],
                device_id=in_plane(o, section), device_id_type=MESH,
            ).start()

    def gather(k, carry):
        left, right = along(RING - k), along(k)

        @pl.when(k > 1)
        def _():
            ring_slots(k, 0, EXPERTS)

        other = jnp.where(k < half, right, z)
        for block in (left, other):
            others = spread_in.at[block, pl.ds(1, EXPERTS - 1)]
            arrived(others, plane_recv.at[block])
        flats = jnp.concatenate(
            [spread_in[left].reshape(rows, FLAT), spread_in[other].reshape(rows, FLAT)], axis=0
        )
        value = jnp.dot(flats, first[:FLAT], preferred_element_type=F32)
        inputs = jnp.concatenate(
            [slots[left].reshape(rows, rest), slots[other].reshape(rows, rest)], axis=0
        )
        value = value + jnp.dot(inputs, first[FLAT:], preferred_element_type=F32)
        hidden[...] = jax.nn.gelu(value, approximate=True).astype(BF16)

        def flat_tile(t, inner):
            cols = pl.ds(pl.multiple_of(t * STEP, STEP), STEP)
            result = jnp.dot(hidden[...], second[:, cols], preferred_element_type=F32)
            result = result.astype(BF16).reshape(2, EXPERTS, capacity, STEP)
            parts_out[left, :, :, cols] = result[0]
            parts_out[other, :, :, cols] = result[1]
            parts_in[left, 0, :, cols] = result[0, 0]
            parts_in[other, 0, :, cols] = result[1, 0]
            return inner

        lax.fori_loop(0, FLAT // STEP, flat_tile, 0)

        @pl.when(k != half - 2)
        def _():
            give_back(left)

        @pl.when((k == half - 3) | (k == half - 1))
        def _():
            give_back(other)

        def tile(t, inner):
            cols = pl.ds(pl.multiple_of(t * STEP, STEP), STEP)
            from_second = pl.ds(pl.multiple_of(FLAT + t * STEP, STEP), STEP)
            result = jnp.dot(hidden[...], second[:, from_second], preferred_element_type=F32)
            result = result.reshape(2, EXPERTS, capacity, STEP)
            partial[left, :, :, cols] = result[0]
            partial[other, :, :, cols] = result[1]
            return inner

        lax.fori_loop(0, rest // STEP, tile, 0)

        @pl.when(k == half - 1)
        def _():
            def early(i, inner):
                pass_on(0, 1, EXPERTS - 1 - 2 * i, False)
                pass_on(1, 1, EXPERTS - 2 - 2 * i, False)
                return inner

            lax.fori_loop(0, EXPERTS // 2, early, 0)

        return carry

    lax.fori_loop(1, half + 1, gather, 0)
    give_back(along(RING - 2))
    give_back(along(2))
    give_back(z)

    def start(i, carry):
        pass_on(0, 0, EXPERTS - 2 - 2 * i, False)
        pass_on(1, 0, EXPERTS - 1 - 2 * i, False)
        return carry

    lax.fori_loop(0, EXPERTS // 2, start, 0)

    def second_hop(i, carry):
        pass_on(0, 1, EXPERTS - 2 - 2 * i, True)
        pass_on(1, 1, EXPERTS - 1 - 2 * i, True)
        return carry

    lax.fori_loop(0, EXPERTS // 2, second_hop, 0)
    for j in range(2, half):
        def later(i, carry):
            pass_on(0, j, EXPERTS - 1 - i, True)
            pass_on(1, j, EXPERTS - 1 - i, True)
            return carry

        lax.fori_loop(0, EXPERTS, later, 0)

    def unpack(block):
        others = parts_in.at[block, pl.ds(1, EXPERTS - 1)]
        arrived(others, parts_recv.at[block])
        picks = routes(block)[:, :rows]
        for c in range(FLAT // STEP):
            cols = slice(c * STEP, (c + 1) * STEP)
            source = parts_in[block, :, :, cols].reshape(rows, STEP)
            value = jnp.dot(picks, source, preferred_element_type=F32)
            whole[block, :, :, cols] = value.reshape(PIECES, piece, STEP)

    def both(k):
        def one(i, carry):
            unpack(along(jnp.where(i == 0, RING - k, k)))
            return carry

        lax.fori_loop(0, 2, one, 0)

    unpack(along(half))
    for c in range(0, PIECES, 2):
        pass_flat(0, 0, c, False)
        pass_flat(1, 0, c + 1, False)
    both(half - 1)
    for c in range(0, PIECES, 2):
        pass_flat(0, 1, c + 1, False)
        pass_flat(1, 1, c, False)
    for c in range(0, PIECES, 2):
        pass_flat(0, 1, c, True)
        pass_flat(1, 1, c + 1, True)

    for o in reversed(range(EXPERTS)):
        value = partial[z, o]
        for way in range(2):
            arrived(arriving.at[way, half - 1, o], sum_recv.at[way, half - 1, o])
            value = value + arriving[way, half - 1, o].astype(F32)
        summed[o] = value.astype(BF16)
        pltpu.make_async_remote_copy(
            src_ref=summed.at[o], dst_ref=returned.at[mirrored(o)],
            send_sem=back_send.at[0], recv_sem=back_recv.at[0],
            device_id=in_plane(o, following), device_id_type=MESH,
        ).start()

    for j in range(2, half):
        both(half - j)
        for c in range(PIECES):
            pass_flat(0, j, c, True)
            pass_flat(1, j, c, True)
    unpack(z)
    for copy in passes:
        copy.wait()
    for c in range(PIECES):
        value = whole[z, c] + act[c * piece:(c + 1) * piece, :FLAT].astype(F32)
        for way in range(2):
            arrived(flat_arriving.at[way, half - 1, c], flat_sum_recv.at[way, half - 1, c])
            value = value + flat_arriving[way, half - 1, c].astype(F32)
        flat_summed[c] = value.astype(BF16)
        pltpu.make_async_remote_copy(
            src_ref=flat_summed.at[c], dst_ref=flat_returned.at[c],
            send_sem=flat_back_send.at[0], recv_sem=flat_back_recv.at[c],
            device_id=(following, me), device_id_type=MESH,
        ).start()

    arrived(returned, back_recv.at[0])
    picks = where_from[:, :rows]
    for c in range(rest // STEP):
        cols = slice(c * STEP, (c + 1) * STEP)
        to = slice(FLAT + c * STEP, FLAT + (c + 1) * STEP)
        mixed = jnp.dot(picks, returned[:, :, cols].reshape(rows, STEP), preferred_element_type=F32)
        out[0, :, to] = (residual[:, cols].astype(F32) + mixed).astype(BF16)
    for c in range(PIECES):
        arrived(flat_returned.at[c], flat_back_recv.at[c])
        out[0, c * piece:(c + 1) * piece, :FLAT] = flat_returned[c]

    arrived(packed.at[pl.ds(1, EXPERTS - 1)], give_send.at[0])
    for way in range(2):
        arrived(slots.at[pl.ds(0, RING - 1)], ring_send.at[way])
    arrived(flat.at[pl.ds(0, RING - 1)], flat_send.at[0])
    arrived(spread_out.at[pl.ds(0, RING - 1)], plane_send.at[0])
    arrived(parts_out.at[pl.ds(0, RING - 1)], parts_send.at[0])
    arrived(flat_sending.at[pl.ds(0, 2 * half * PIECES - PIECES)], flat_sum_send.at[0])
    arrived(summed, back_send.at[0])
    arrived(flat_summed, flat_back_send.at[0])


def per_device(sections, n, activations, norm_gain, in_proj, out_proj, expert_ids):
    tokens, width = activations.shape[1:]
    ff = in_proj.shape[2]
    capacity = 2 * tokens // EXPERTS
    rows = EXPERTS * capacity
    rest, piece, half = width - FLAT, tokens // PIECES, RING // 2
    dma = pltpu.SemaphoreType.DMA
    vmem = pltpu.VMEM
    return pl.pallas_call(
        functools.partial(kernel, sections, n, capacity),
        out_shape=pltpu.VMEM(activations.shape, activations.dtype),
        in_specs=[pl.BlockSpec(memory_space=pl.ANY)] * 5,
        out_specs=pl.BlockSpec(memory_space=pltpu.VMEM),
        scratch_shapes=[
            vmem((tokens, width), BF16),
            vmem((1, width), F32),
            vmem((1, tokens), jnp.int32),
            vmem((width, ff), BF16),
            vmem((ff, width), BF16),
            vmem((tokens, rest), BF16),
            vmem((EXPERTS, capacity, rest), BF16),
            vmem((RING, EXPERTS, capacity, rest), BF16),
            vmem((RING, PIECES, piece, FLAT + LANES), BF16),
            vmem((RING, EXPERTS, capacity, FLAT), BF16),
            vmem((RING, EXPERTS, capacity, FLAT), BF16),
            vmem((2 * rows, ff), BF16),
            vmem((RING, EXPERTS, capacity, rest), F32),
            vmem((2, half, EXPERTS, capacity, rest), BF16),
            vmem((2, half, EXPERTS, capacity, rest), BF16),
            vmem((EXPERTS, capacity, rest), BF16),
            vmem((EXPERTS, capacity, rest), BF16),
            vmem((RING, EXPERTS, capacity, FLAT), BF16),
            vmem((RING, EXPERTS, capacity, FLAT), BF16),
            vmem((RING, PIECES, piece, FLAT), F32),
            vmem((2 * half * PIECES, piece, FLAT), BF16),
            vmem((2, half, PIECES, piece, FLAT), BF16),
            vmem((PIECES, piece, FLAT), BF16),
            vmem((PIECES, piece, FLAT), BF16),
            vmem((tokens, LANES), BF16),
            vmem((tokens, rest), BF16),
            vmem((tokens, LANES), BF16),
            dma((3,)),
            dma((2,)),
            dma((2,)),
            dma((2,)),
            dma((1,)),
            dma((2,)),
            dma((RING, EXPERTS)),
            dma((2, half, EXPERTS)),
            dma((1,)),
            dma((1,)),
            dma((1,)),
            dma((RING, PIECES)),
            dma((1,)),
            dma((RING,)),
            dma((1,)),
            dma((RING,)),
            dma((1,)),
            dma((2, half, PIECES)),
            dma((1,)),
            dma((PIECES,)),
        ],
        compiler_params=pltpu.CompilerParams(
            collective_id=0, has_side_effects=True, vmem_limit_bytes=62 * 1024 * 1024
        ),
    )(activations, norm_gain, expert_ids.reshape(1, tokens), in_proj, out_proj)


def solution(mesh):
    return jax.shard_map(
        functools.partial(per_device, mesh.shape["section"], mesh.shape["expert"]),
        mesh=mesh,
        in_specs=(
            P("section", "expert", None),
            P("section", None),
            P("section", None, "expert"),
            P("section", "expert", None),
            P("section", "expert", None),
        ),
        out_specs=P("section", "expert", None),
        check_vma=False,
    )
```

```python
import functools

import jax
import jax.numpy as jnp
from jax import lax
from jax.experimental import pallas as pl
from jax.experimental.pallas import tpu as pltpu
from jax.sharding import PartitionSpec as P

EXPERTS = 8
RING = 8
NX = 4
FLAT = 2048
PIECES = 4
LANES = 128
STEP = 512
NEAR = ((0, 0), (0, 1), (0, 3), (1, 0), (0, 2), (1, 1), (1, 3), (1, 2))
MESH = pl.DeviceIdType.MESH
F32, BF16 = jnp.float32, jnp.bfloat16

epsilon = 1e-06


def neighbour(group, o):
    dy, dx = NEAR[o]
    return lax.rem(group // NX + dy, EXPERTS // NX) * NX + lax.rem(group % NX + dx, NX)


def mirrored(o):
    dy, dx = NEAR[o]
    return NEAR.index((dy, (NX - dx) % NX))


def placement(routed, ranks, capacity, group, rows):
    row = lax.broadcasted_iota(jnp.int32, (rows, routed.shape[1]), 0)
    place = row // capacity
    owner = jnp.full_like(place, -1)
    for o in range(EXPERTS):
        owner = jnp.where(place == o, neighbour(group, o), owner)
    return jnp.where((owner == routed) & (row % capacity == ranks), 1.0, 0.0).astype(F32)


def arrived(ref, sem):
    pltpu.make_async_copy(ref, ref, sem).wait()


def kernel(
    sections, n, capacity, act_hbm, gain_hbm, ids_hbm, first_hbm, second_hbm, out,
    act, gain, ids, first, second, normed, packed, slots, flat, spread_out, spread_in, total, hidden,
    partial, sending, arriving, summed, returned,
    parts_out, parts_in, whole, flat_sending, flat_arriving, flat_summed, flat_returned,
    where_to, residual, where_from,
    small_sem, weight_sem, pass_send, pass_recv, give_send, ring_send, ring_recv, sum_recv, back_send, back_recv,
    flat_send, flat_recv, plane_send, plane_recv, parts_send, parts_recv, flat_sum_send, flat_sum_recv,
    flat_back_send, flat_back_recv,
):
    section, me = lax.axis_index("section"), lax.axis_index("expert")
    following, leading = lax.rem(section + 1, sections), lax.rem(section + sections - 1, sections)
    group, z = me // RING, lax.rem(me, RING)
    tokens, width = act.shape
    rows = EXPERTS * capacity
    rest = width - FLAT
    half = RING // 2
    piece = tokens // PIECES
    last = RING - 1

    def along(k):
        return lax.rem(z + k, RING)

    def on_ring(k):
        return (section, group * RING + along(k))

    def in_plane(o, which):
        return (which, neighbour(group, o) * RING + z)

    smalls = [
        pltpu.make_async_copy(act_hbm.at[0], act, small_sem.at[0]),
        pltpu.make_async_copy(gain_hbm, gain, small_sem.at[1]),
        pltpu.make_async_copy(ids_hbm, ids, small_sem.at[2]),
    ]
    weights = [
        pltpu.make_async_copy(first_hbm.at[0], first, weight_sem.at[0]),
        pltpu.make_async_copy(second_hbm.at[0], second, weight_sem.at[1]),
    ]
    for copy in smalls:
        copy.start()
    barrier = pltpu.get_barrier_semaphore()
    greeted = [in_plane(o, section) for o in range(1, EXPERTS)] + [on_ring(1), on_ring(last)]
    greeted += [in_plane(o, leading) for o in range(EXPERTS)]
    for peer in greeted:
        pl.semaphore_signal(barrier, inc=1, device_id=peer, device_id_type=MESH)
    for copy in smalls:
        copy.wait()
    for copy in weights:
        copy.start()

    floats = act[...].astype(F32)
    scale = lax.rsqrt(jnp.mean(floats * floats, axis=-1, keepdims=True) + epsilon)
    values = (floats * scale * gain[...]).astype(BF16)
    normed[...] = values[:, FLAT:]
    flat[z, :, :, :FLAT] = values[:, :FLAT].reshape(PIECES, piece, FLAT)
    routed = ids[...]
    expert = lax.broadcasted_iota(jnp.int32, (EXPERTS, tokens), 0)
    onehot = jnp.where(expert == routed, 1.0, 0.0).astype(F32)
    earlier = lax.broadcasted_iota(jnp.int32, (tokens, tokens), 0) < lax.broadcasted_iota(
        jnp.int32, (tokens, tokens), 1
    )
    before = jnp.dot(
        onehot.astype(BF16), jnp.where(earlier, 1.0, 0.0).astype(BF16), preferred_element_type=F32
    )
    ranks = jnp.sum(before * onehot, axis=0, keepdims=True).astype(jnp.int32)
    placing = placement(routed, ranks, capacity, group, LANES)
    back = placing.T.astype(BF16)
    where_to[...] = back
    flat[z, :, :, FLAT:] = back.reshape(PIECES, piece, LANES)
    placing = placing[:rows].astype(BF16)

    pl.semaphore_wait(barrier, len(greeted))

    def forward_flat(block, c, k):
        pltpu.make_async_remote_copy(
            src_ref=flat.at[block, c], dst_ref=flat.at[block, c],
            send_sem=flat_send.at[0], recv_sem=flat_recv.at[block, c],
            device_id=on_ring(k), device_id_type=MESH,
        ).start()

    def forward(block, o, k, way):
        pltpu.make_async_remote_copy(
            src_ref=slots.at[block, o], dst_ref=slots.at[block, o],
            send_sem=ring_send.at[way], recv_sem=ring_recv.at[block, o],
            device_id=on_ring(k), device_id_type=MESH,
        ).start()

    for c in range(PIECES):
        forward_flat(z, c, 1)
        forward_flat(z, c, last)

    for c in range(rest // STEP):
        cols = slice(c * STEP, (c + 1) * STEP)
        block = jnp.dot(placing, normed[:, cols], preferred_element_type=F32)
        packed[:, :, cols] = block.astype(BF16).reshape(EXPERTS, capacity, STEP)
    slots[z, 0] = packed[0]
    for o in range(1, EXPERTS):
        pltpu.make_async_remote_copy(
            src_ref=packed.at[o], dst_ref=slots.at[z, mirrored(o)],
            send_sem=give_send.at[0], recv_sem=ring_recv.at[z, mirrored(o)],
            device_id=in_plane(o, section), device_id_type=MESH,
        ).start()
    forward(z, 0, 1, 0)
    forward(z, 0, last, 1)

    def routes(block):
        return flat[block, :, :, FLAT:].reshape(tokens, LANES)

    def pack(block):
        to_slot = routes(block).astype(F32).T[:rows].astype(BF16)
        for c in range(FLAT // STEP):
            cols = slice(c * STEP, (c + 1) * STEP)
            source = flat[block, :, :, cols].reshape(tokens, STEP)
            value = jnp.dot(to_slot, source, preferred_element_type=F32)
            value = value.astype(BF16).reshape(EXPERTS, capacity, STEP)
            spread_out[block, :, :, cols] = value
            spread_in[block, 0, :, cols] = value[0]
        for o in range(1, EXPERTS):
            pltpu.make_async_remote_copy(
                src_ref=spread_out.at[block, o], dst_ref=spread_in.at[block, mirrored(o)],
                send_sem=plane_send.at[0], recv_sem=plane_recv.at[block],
                device_id=in_plane(o, section), device_id_type=MESH,
            ).start()

    pack(z)
    passes = [
        pltpu.make_async_remote_copy(
            src_ref=src, dst_ref=dst, send_sem=pass_send.at[k], recv_sem=pass_recv.at[k],
            device_id=(following, me), device_id_type=MESH,
        )
        for k, (src, dst) in enumerate(((act.at[:, pl.ds(FLAT, rest)], residual), (where_to, where_from)))
    ]
    for copy in passes:
        copy.start()

    def spread(o):
        arrived(slots.at[z, o], ring_recv.at[z, o])
        forward(z, o, 1, 0)
        forward(z, o, last, 1)

    def ring_slot(k, o):
        left, right = along(RING - k), along(k)
        arrived(slots.at[left, o], ring_recv.at[left, o])

        @pl.when((k < half - 1) | ((k == half - 1) & (o % 2 == 0)))
        def _():
            forward(left, o, 1, 0)

        @pl.when(k < half)
        def _():
            arrived(slots.at[right, o], ring_recv.at[right, o])

        @pl.when((k < half - 1) | ((k == half - 1) & (o % 2 == 1)))
        def _():
            forward(right, o, last, 1)

    def ring_flat(k, beside):
        left, right = along(RING - k), along(k)

        def hop(c, inner):
            arrived(flat.at[left, c], flat_recv.at[left, c])
            if k < half - 1:
                forward_flat(left, c, 1)
            if k < half:
                arrived(flat.at[right, c], flat_recv.at[right, c])
            if k < half - 1:
                forward_flat(right, c, last)
            if k == half - 1:
                @pl.when(c % 2 == 0)
                def _():
                    forward_flat(left, c, 1)

                @pl.when(c % 2 == 1)
                def _():
                    forward_flat(right, c, last)

            beside(c)
            return inner

        lax.fori_loop(0, PIECES, hop, 0)

        def fill(i, inner):
            pack(along(jnp.where(i == 0, RING - k, k)))
            return inner

        lax.fori_loop(0, 2 if k < half else 1, fill, 0)

    def near(c):
        @pl.when(c > 0)
        def _():
            spread(c)

    ring_flat(1, near)
    ring_flat(2, lambda c: spread(PIECES + c))
    ring_flat(3, lambda c: ring_slot(jnp.int32(1), c))
    ring_flat(4, lambda c: ring_slot(jnp.int32(1), PIECES + c))
    for copy in weights:
        copy.wait()

    def pass_on(way, j, o, add):
        distance = half - j
        block = along(distance if way == 0 else RING - distance)
        value = partial[block, o]
        if add:
            arrived(arriving.at[way, j - 1, o], sum_recv.at[way, j - 1, o])
            value = value + arriving[way, j - 1, o].astype(F32)
        sending[way, j, o] = value.astype(BF16)
        pltpu.make_async_remote_copy(
            src_ref=sending.at[way, j, o], dst_ref=arriving.at[way, j, o],
            send_sem=ring_send.at[way], recv_sem=sum_recv.at[way, j, o],
            device_id=on_ring(1 if way == 0 else last), device_id_type=MESH,
        ).start()

    def pass_flat(way, j, c, add):
        distance = half - j
        block = along(distance if way == 0 else RING - distance)
        value = whole[block, c]
        if add:
            arrived(flat_arriving.at[way, j - 1, c], flat_sum_recv.at[way, j - 1, c])
            value = value + flat_arriving[way, j - 1, c].astype(F32)
        place = (way * half + j) * PIECES + c
        flat_sending[place] = value.astype(BF16)
        pltpu.make_async_remote_copy(
            src_ref=flat_sending.at[place], dst_ref=flat_arriving.at[way, j, c],
            send_sem=flat_sum_send.at[0], recv_sem=flat_sum_recv.at[way, j, c],
            device_id=on_ring(1 if way == 0 else last), device_id_type=MESH,
        ).start()

    def give_back(block):
        for o in range(1, EXPERTS):
            pltpu.make_async_remote_copy(
                src_ref=parts_out.at[block, o], dst_ref=parts_in.at[block, mirrored(o)],
                send_sem=parts_send.at[0], recv_sem=parts_recv.at[block],
                device_id=in_plane(o, section), device_id_type=MESH,
            ).start()

    def first_flat(left, other):
        for block in (left, other):
            others = spread_in.at[block, pl.ds(1, EXPERTS - 1)]
            arrived(others, plane_recv.at[block])
        inputs = jnp.concatenate(
            [spread_in[left].reshape(rows, FLAT), spread_in[other].reshape(rows, FLAT)], axis=0
        )
        total[...] = jnp.dot(inputs, first[:FLAT], preferred_element_type=F32)

    def first_slots(left, other):
        inputs = jnp.concatenate(
            [slots[left].reshape(rows, rest), slots[other].reshape(rows, rest)], axis=0
        )
        value = total[...] + jnp.dot(inputs, first[FLAT:], preferred_element_type=F32)
        hidden[...] = jax.nn.gelu(value, approximate=True).astype(BF16)

    def second_flat(left, other, low, high):
        def tile(t, inner):
            cols = pl.ds(pl.multiple_of(t * STEP, STEP), STEP)
            result = jnp.dot(hidden[...], second[:, cols], preferred_element_type=F32)
            result = result.astype(BF16).reshape(2, EXPERTS, capacity, STEP)
            parts_out[left, :, :, cols] = result[0]
            parts_out[other, :, :, cols] = result[1]
            parts_in[left, 0, :, cols] = result[0, 0]
            parts_in[other, 0, :, cols] = result[1, 0]
            return inner

        lax.fori_loop(low, high, tile, 0)

    def second_slots(left, other, low, high):
        def tile(t, inner):
            cols = pl.ds(pl.multiple_of(t * STEP, STEP), STEP)
            from_second = pl.ds(pl.multiple_of(FLAT + t * STEP, STEP), STEP)
            result = jnp.dot(hidden[...], second[:, from_second], preferred_element_type=F32)
            result = result.reshape(2, EXPERTS, capacity, STEP)
            partial[left, :, :, cols] = result[0]
            partial[other, :, :, cols] = result[1]
            return inner

        lax.fori_loop(low, high, tile, 0)

    flat_tiles, slot_tiles = FLAT // STEP, rest // STEP

    def stage(k, carry):
        left, right = along(RING - (k - 1)), along(k - 1)

        def hop(o, inner):
            ring_slot(k, o)

            @pl.when(o == 0)
            def _():
                first_flat(left, right)

            @pl.when(o == 1)
            def _():
                first_slots(left, right)

            @pl.when((o > 1) & (o < 6))
            def _():
                i = o - 2
                second_flat(left, right, i * flat_tiles // 4, (i + 1) * flat_tiles // 4)
                second_slots(left, right, i * slot_tiles // 4, (i + 1) * slot_tiles // 4)

            return inner

        lax.fori_loop(0, EXPERTS, hop, 0)

        @pl.when(k == 2)
        def _():
            give_back(left)
            give_back(right)

        return carry

    lax.fori_loop(2, half, stage, 0)

    def finish(k, carry):
        left, right = along(RING - k), along(k)
        other = jnp.where(k < half, right, z)

        @pl.when(k == half)
        def _():
            def land(o, inner):
                arrived(slots.at[left, o], ring_recv.at[left, o])
                return inner

            lax.fori_loop(0, EXPERTS, land, 0)

        first_flat(left, other)
        first_slots(left, other)
        second_slots(left, other, 0, slot_tiles)

        def early(i, inner):
            pass_on(0, 1, EXPERTS - 1 - 2 * i, False)
            pass_on(1, 1, EXPERTS - 2 - 2 * i, False)
            return inner

        def start(i, inner):
            pass_on(0, 0, EXPERTS - 2 - 2 * i, False)
            pass_on(1, 0, EXPERTS - 1 - 2 * i, False)
            return inner

        @pl.when(k == half - 1)
        def _():
            lax.fori_loop(0, EXPERTS // 2, early, 0)

        @pl.when(k == half)
        def _():
            lax.fori_loop(0, EXPERTS // 2, start, 0)

        second_flat(left, other, 0, flat_tiles)
        give_back(left)

        @pl.when(k == half - 1)
        def _():
            give_back(other)

        return carry

    lax.fori_loop(half - 1, half + 1, finish, 0)
    give_back(along(RING - 2))
    give_back(along(2))
    give_back(z)

    def second_hop(i, carry):
        pass_on(0, 1, EXPERTS - 2 - 2 * i, True)
        pass_on(1, 1, EXPERTS - 1 - 2 * i, True)
        return carry

    lax.fori_loop(0, EXPERTS // 2, second_hop, 0)

    def later(j):
        def one(i, carry):
            pass_on(0, j, EXPERTS - 1 - i, True)
            pass_on(1, j, EXPERTS - 1 - i, True)
            return carry

        lax.fori_loop(0, EXPERTS, one, 0)

    def later_flat(j):
        def one(c, carry):
            pass_flat(0, j, c, True)
            pass_flat(1, j, c, True)
            return carry

        lax.fori_loop(0, PIECES, one, 0)

    def unpack(block):
        others = parts_in.at[block, pl.ds(1, EXPERTS - 1)]
        arrived(others, parts_recv.at[block])
        picks = routes(block)[:, :rows]
        for c in range(FLAT // STEP):
            cols = slice(c * STEP, (c + 1) * STEP)
            source = parts_in[block, :, :, cols].reshape(rows, STEP)
            value = jnp.dot(picks, source, preferred_element_type=F32)
            whole[block, :, :, cols] = value.reshape(PIECES, piece, STEP)

    def both(k):
        def one(i, carry):
            unpack(along(jnp.where(i == 0, RING - k, k)))
            return carry

        lax.fori_loop(0, 2, one, 0)

    later(2)
    unpack(along(half))
    for c in range(0, PIECES, 2):
        pass_flat(0, 0, c, False)
        pass_flat(1, 0, c + 1, False)
    both(half - 1)
    for c in range(0, PIECES, 2):
        pass_flat(0, 1, c + 1, False)
        pass_flat(1, 1, c, False)
    later(3)
    for c in range(0, PIECES, 2):
        pass_flat(0, 1, c, True)
        pass_flat(1, 1, c + 1, True)
    both(2)
    later_flat(2)

    for o in reversed(range(EXPERTS)):
        value = partial[z, o]
        for way in range(2):
            arrived(arriving.at[way, half - 1, o], sum_recv.at[way, half - 1, o])
            value = value + arriving[way, half - 1, o].astype(F32)
        summed[o] = value.astype(BF16)
        pltpu.make_async_remote_copy(
            src_ref=summed.at[o], dst_ref=returned.at[mirrored(o)],
            send_sem=back_send.at[0], recv_sem=back_recv.at[0],
            device_id=in_plane(o, following), device_id_type=MESH,
        ).start()

    both(1)
    later_flat(3)
    unpack(z)
    for copy in passes:
        copy.wait()
    for c in range(PIECES):
        value = whole[z, c] + act[c * piece:(c + 1) * piece, :FLAT].astype(F32)
        for way in range(2):
            arrived(flat_arriving.at[way, half - 1, c], flat_sum_recv.at[way, half - 1, c])
            value = value + flat_arriving[way, half - 1, c].astype(F32)
        flat_summed[c] = value.astype(BF16)
        pltpu.make_async_remote_copy(
            src_ref=flat_summed.at[c], dst_ref=flat_returned.at[c],
            send_sem=flat_back_send.at[0], recv_sem=flat_back_recv.at[c],
            device_id=(following, me), device_id_type=MESH,
        ).start()

    arrived(returned, back_recv.at[0])
    picks = where_from[:, :rows]
    for c in range(rest // STEP):
        cols = slice(c * STEP, (c + 1) * STEP)
        to = slice(FLAT + c * STEP, FLAT + (c + 1) * STEP)
        mixed = jnp.dot(picks, returned[:, :, cols].reshape(rows, STEP), preferred_element_type=F32)
        out[0, :, to] = (residual[:, cols].astype(F32) + mixed).astype(BF16)
    for c in range(PIECES):
        arrived(flat_returned.at[c], flat_back_recv.at[c])
        out[0, c * piece:(c + 1) * piece, :FLAT] = flat_returned[c]

    arrived(packed.at[pl.ds(1, EXPERTS - 1)], give_send.at[0])
    for way in range(2):
        arrived(slots.at[pl.ds(0, RING - 1)], ring_send.at[way])
    arrived(flat.at[pl.ds(0, RING - 1)], flat_send.at[0])
    arrived(spread_out.at[pl.ds(0, RING - 1)], plane_send.at[0])
    arrived(parts_out.at[pl.ds(0, RING - 1)], parts_send.at[0])
    arrived(flat_sending.at[pl.ds(0, 2 * half * PIECES - PIECES)], flat_sum_send.at[0])
    arrived(summed, back_send.at[0])
    arrived(flat_summed, flat_back_send.at[0])


def per_device(sections, n, activations, norm_gain, in_proj, out_proj, expert_ids):
    tokens, width = activations.shape[1:]
    ff = in_proj.shape[2]
    capacity = 2 * tokens // EXPERTS
    rows = EXPERTS * capacity
    rest, piece, half = width - FLAT, tokens // PIECES, RING // 2
    dma = pltpu.SemaphoreType.DMA
    vmem = pltpu.VMEM
    return pl.pallas_call(
        functools.partial(kernel, sections, n, capacity),
        out_shape=pltpu.VMEM(activations.shape, activations.dtype),
        in_specs=[pl.BlockSpec(memory_space=pl.ANY)] * 5,
        out_specs=pl.BlockSpec(memory_space=pltpu.VMEM),
        scratch_shapes=[
            vmem((tokens, width), BF16),
            vmem((1, width), F32),
            vmem((1, tokens), jnp.int32),
            vmem((width, ff), BF16),
            vmem((ff, width), BF16),
            vmem((tokens, rest), BF16),
            vmem((EXPERTS, capacity, rest), BF16),
            vmem((RING, EXPERTS, capacity, rest), BF16),
            vmem((RING, PIECES, piece, FLAT + LANES), BF16),
            vmem((RING, EXPERTS, capacity, FLAT), BF16),
            vmem((RING, EXPERTS, capacity, FLAT), BF16),
            vmem((2 * rows, ff), F32),
            vmem((2 * rows, ff), BF16),
            vmem((RING, EXPERTS, capacity, rest), F32),
            vmem((2, half, EXPERTS, capacity, rest), BF16),
            vmem((2, half, EXPERTS, capacity, rest), BF16),
            vmem((EXPERTS, capacity, rest), BF16),
            vmem((EXPERTS, capacity, rest), BF16),
            vmem((RING, EXPERTS, capacity, FLAT), BF16),
            vmem((RING, EXPERTS, capacity, FLAT), BF16),
            vmem((RING, PIECES, piece, FLAT), F32),
            vmem((2 * half * PIECES, piece, FLAT), BF16),
            vmem((2, half, PIECES, piece, FLAT), BF16),
            vmem((PIECES, piece, FLAT), BF16),
            vmem((PIECES, piece, FLAT), BF16),
            vmem((tokens, LANES), BF16),
            vmem((tokens, rest), BF16),
            vmem((tokens, LANES), BF16),
            dma((3,)),
            dma((2,)),
            dma((2,)),
            dma((2,)),
            dma((1,)),
            dma((2,)),
            dma((RING, EXPERTS)),
            dma((2, half, EXPERTS)),
            dma((1,)),
            dma((1,)),
            dma((1,)),
            dma((RING, PIECES)),
            dma((1,)),
            dma((RING,)),
            dma((1,)),
            dma((RING,)),
            dma((1,)),
            dma((2, half, PIECES)),
            dma((1,)),
            dma((PIECES,)),
        ],
        compiler_params=pltpu.CompilerParams(
            collective_id=0, has_side_effects=True, vmem_limit_bytes=62 * 1024 * 1024
        ),
    )(activations, norm_gain, expert_ids.reshape(1, tokens), in_proj, out_proj)


def solution(mesh):
    return jax.shard_map(
        functools.partial(per_device, mesh.shape["section"], mesh.shape["expert"]),
        mesh=mesh,
        in_specs=(
            P("section", "expert", None),
            P("section", None),
            P("section", None, "expert"),
            P("section", "expert", None),
            P("section", "expert", None),
        ),
        out_specs=P("section", "expert", None),
        check_vma=False,
    )
```

```python
import functools

import jax
import jax.numpy as jnp
from jax import lax
from jax.experimental import pallas as pl
from jax.experimental.pallas import tpu as pltpu
from jax.sharding import PartitionSpec as P

EXPERTS = 8
RING = 8
NX = 4
FLAT = 2176
BACK = 2048
PIECES = 4
LANES = 128
FIRST_PACK, SLOT_PACK = 2176, 640
BACK_STEP, SLOT_STEP = 2048, 1024
NEAR = ((0, 0), (0, 1), (0, 3), (1, 0), (0, 2), (1, 1), (1, 3), (1, 2))
MESH = pl.DeviceIdType.MESH
F32, BF16 = jnp.float32, jnp.bfloat16

epsilon = 1e-06


def neighbour(group, o):
    dy, dx = NEAR[o]
    return lax.rem(group // NX + dy, EXPERTS // NX) * NX + lax.rem(group % NX + dx, NX)


def mirrored(o):
    dy, dx = NEAR[o]
    return NEAR.index((dy, (NX - dx) % NX))


def placement(routed, ranks, capacity, group, rows):
    row = lax.broadcasted_iota(jnp.int32, (rows, routed.shape[1]), 0)
    place = row // capacity
    owner = jnp.full_like(place, -1)
    for o in range(EXPERTS):
        owner = jnp.where(place == o, neighbour(group, o), owner)
    return jnp.where((owner == routed) & (row % capacity == ranks), 1.0, 0.0).astype(F32)


def arrived(ref, sem):
    pltpu.make_async_copy(ref, ref, sem).wait()


def kernel(
    sections, n, capacity, act_hbm, gain_hbm, ids_hbm, first_hbm, second_hbm, out,
    act, gain, ids, first, second, normed, packed, slots, flat, spread_out, spread_in, total, hidden,
    partial, sending, arriving, summed, returned,
    parts_out, parts_in, whole, flat_sending, flat_arriving, flat_summed, flat_returned,
    where_to, residual, where_from,
    small_sem, weight_sem, pass_send, pass_recv, give_send, ring_send, ring_recv, sum_send, back_send, back_recv,
    flat_send, flat_recv, plane_send, plane_recv, parts_send, parts_recv, flat_sum_send,
    flat_back_send, flat_back_recv,
):
    section, me = lax.axis_index("section"), lax.axis_index("expert")
    following, leading = lax.rem(section + 1, sections), lax.rem(section + sections - 1, sections)
    group, z = me // RING, lax.rem(me, RING)
    tokens, width = act.shape
    rows = EXPERTS * capacity
    rest, back_rest = width - FLAT, width - BACK
    half = RING // 2
    piece = tokens // PIECES
    last = RING - 1

    def along(k):
        return lax.rem(z + k, RING)

    def on_ring(k):
        return (section, group * RING + along(k))

    def in_plane(o, which):
        return (which, neighbour(group, o) * RING + z)

    smalls = [
        pltpu.make_async_copy(act_hbm.at[0], act, small_sem.at[0]),
        pltpu.make_async_copy(gain_hbm, gain, small_sem.at[1]),
        pltpu.make_async_copy(ids_hbm, ids, small_sem.at[2]),
    ]
    weights = [
        pltpu.make_async_copy(first_hbm.at[0], first, weight_sem.at[0]),
        pltpu.make_async_copy(second_hbm.at[0], second, weight_sem.at[1]),
    ]
    for copy in smalls:
        copy.start()
    barrier = pltpu.get_barrier_semaphore()
    greeted = [in_plane(o, section) for o in range(1, EXPERTS)] + [on_ring(1), on_ring(last)]
    greeted += [in_plane(o, leading) for o in range(EXPERTS)]
    for peer in greeted:
        pl.semaphore_signal(barrier, inc=1, device_id=peer, device_id_type=MESH)
    for copy in smalls:
        copy.wait()
    for copy in weights:
        copy.start()

    floats = act[...].astype(F32)
    scale = lax.rsqrt(jnp.mean(floats * floats, axis=-1, keepdims=True) + epsilon)
    values = (floats * scale * gain[...]).astype(BF16)
    normed[...] = values[:, FLAT:]
    flat[z, :, :, :FLAT] = values[:, :FLAT].reshape(PIECES, piece, FLAT)
    routed = ids[...]
    expert = lax.broadcasted_iota(jnp.int32, (EXPERTS, tokens), 0)
    onehot = jnp.where(expert == routed, 1.0, 0.0).astype(F32)
    earlier = lax.broadcasted_iota(jnp.int32, (tokens, tokens), 0) < lax.broadcasted_iota(
        jnp.int32, (tokens, tokens), 1
    )
    before = jnp.dot(
        onehot.astype(BF16), jnp.where(earlier, 1.0, 0.0).astype(BF16), preferred_element_type=F32
    )
    ranks = jnp.sum(before * onehot, axis=0, keepdims=True).astype(jnp.int32)
    placing = placement(routed, ranks, capacity, group, LANES)
    back = placing.T.astype(BF16)
    where_to[...] = back
    flat[z, :, :, FLAT:] = back.reshape(PIECES, piece, LANES)
    placing = placing[:rows].astype(BF16)

    pl.semaphore_wait(barrier, len(greeted))

    def forward_flat(block, c, k):
        pltpu.make_async_remote_copy(
            src_ref=flat.at[block, c], dst_ref=flat.at[block, c],
            send_sem=flat_send.at[0], recv_sem=flat_recv.at[block, c],
            device_id=on_ring(k), device_id_type=MESH,
        ).start()

    def forward(block, o, k):
        pltpu.make_async_remote_copy(
            src_ref=slots.at[block, o], dst_ref=slots.at[block, o],
            send_sem=ring_send.at[0], recv_sem=ring_recv.at[block, o],
            device_id=on_ring(k), device_id_type=MESH,
        ).start()

    for c in range(PIECES):
        forward_flat(z, c, 1)
        forward_flat(z, c, last)

    for c in range(rest // SLOT_PACK):
        cols = slice(c * SLOT_PACK, (c + 1) * SLOT_PACK)
        block = jnp.dot(placing, normed[:, cols], preferred_element_type=F32)
        packed[:, :, cols] = block.astype(BF16).reshape(EXPERTS, capacity, SLOT_PACK)
    slots[z, 0] = packed[0]
    for o in range(1, EXPERTS):
        pltpu.make_async_remote_copy(
            src_ref=packed.at[o], dst_ref=slots.at[z, mirrored(o)],
            send_sem=give_send.at[0], recv_sem=ring_recv.at[z, mirrored(o)],
            device_id=in_plane(o, section), device_id_type=MESH,
        ).start()
    forward(z, 0, 1)
    forward(z, 0, last)

    def routes(block):
        return flat[block, :, :, FLAT:].reshape(tokens, LANES)

    def pack(block):
        to_slot = routes(block).astype(F32).T[:rows].astype(BF16)
        for c in range(FLAT // FIRST_PACK):
            cols = slice(c * FIRST_PACK, (c + 1) * FIRST_PACK)
            source = flat[block, :, :, cols].reshape(tokens, FIRST_PACK)
            value = jnp.dot(to_slot, source, preferred_element_type=F32)
            value = value.astype(BF16).reshape(EXPERTS, capacity, FIRST_PACK)
            spread_out[block, :, :, cols] = value
            spread_in[block, 0, :, cols] = value[0]
        for o in range(1, EXPERTS):
            pltpu.make_async_remote_copy(
                src_ref=spread_out.at[block, o], dst_ref=spread_in.at[block, mirrored(o)],
                send_sem=plane_send.at[0], recv_sem=plane_recv.at[block],
                device_id=in_plane(o, section), device_id_type=MESH,
            ).start()

    pack(z)
    passes = [
        pltpu.make_async_remote_copy(
            src_ref=src, dst_ref=dst, send_sem=pass_send.at[k], recv_sem=pass_recv.at[k],
            device_id=(following, me), device_id_type=MESH,
        )
        for k, (src, dst) in enumerate(((act.at[:, pl.ds(BACK, back_rest)], residual), (where_to, where_from)))
    ]
    for copy in passes:
        copy.start()

    def spread(o):
        arrived(slots.at[z, o], ring_recv.at[z, o])
        forward(z, o, 1)
        forward(z, o, last)

    def ring_slot(k, o):
        left, right = along(RING - k), along(k)
        arrived(slots.at[left, o], ring_recv.at[left, o])

        @pl.when((k < half - 1) | ((k == half - 1) & (o % 2 == 0)))
        def _():
            forward(left, o, 1)

        @pl.when(k < half)
        def _():
            arrived(slots.at[right, o], ring_recv.at[right, o])

        @pl.when((k < half - 1) | ((k == half - 1) & (o % 2 == 1)))
        def _():
            forward(right, o, last)

    def ring_flat(k, beside):
        left, right = along(RING - k), along(k)

        def hop(c, inner):
            arrived(flat.at[left, c], flat_recv.at[left, c])
            if k < half - 1:
                forward_flat(left, c, 1)
            if k < half:
                arrived(flat.at[right, c], flat_recv.at[right, c])
            if k < half - 1:
                forward_flat(right, c, last)
            if k == half - 1:
                @pl.when(c % 2 == 0)
                def _():
                    forward_flat(left, c, 1)

                @pl.when(c % 2 == 1)
                def _():
                    forward_flat(right, c, last)

            beside(c)
            return inner

        lax.fori_loop(0, PIECES, hop, 0)

        def fill(i, inner):
            pack(along(jnp.where(i == 0, RING - k, k)))
            return inner

        lax.fori_loop(0, 2 if k < half else 1, fill, 0)

    def near(c):
        @pl.when(c > 0)
        def _():
            spread(c)

    ring_flat(1, near)
    ring_flat(2, lambda c: spread(PIECES + c))
    ring_flat(3, lambda c: ring_slot(jnp.int32(1), c))
    ring_flat(4, lambda c: ring_slot(jnp.int32(1), PIECES + c))
    for copy in weights:
        copy.wait()

    def sum_sem(way, j, o, shift):
        return ring_recv.at[along((j + shift) if way == 0 else (2 * RING - j - shift)), o]

    def flat_sum_sem(way, j, c):
        return flat_recv.at[way * half + j, c]

    def pass_on(way, j, o, add):
        distance = half - j
        block = along(distance if way == 0 else RING - distance)
        value = partial[block, o]
        if add:
            arrived(arriving.at[way, j - 1, o], sum_sem(way, j - 1, o, 0))
            value = value + arriving[way, j - 1, o].astype(F32)
        place = (way * half + j) * EXPERTS + o
        sending[place] = value.astype(BF16)
        pltpu.make_async_remote_copy(
            src_ref=sending.at[place], dst_ref=arriving.at[way, j, o],
            send_sem=sum_send.at[0], recv_sem=sum_sem(way, j, o, 1),
            device_id=on_ring(1 if way == 0 else last), device_id_type=MESH,
        ).start()

    def pass_flat(way, j, c, add):
        distance = half - j
        block = along(distance if way == 0 else RING - distance)
        value = whole[block, c]
        if add:
            arrived(flat_arriving.at[way, j - 1, c], flat_sum_sem(way, j - 1, c))
            value = value + flat_arriving[way, j - 1, c].astype(F32)
        place = (way * half + j) * PIECES + c
        flat_sending[place] = value.astype(BF16)
        pltpu.make_async_remote_copy(
            src_ref=flat_sending.at[place], dst_ref=flat_arriving.at[way, j, c],
            send_sem=flat_sum_send.at[0], recv_sem=flat_sum_sem(way, j, c),
            device_id=on_ring(1 if way == 0 else last), device_id_type=MESH,
        ).start()

    def give_back(block):
        for o in range(1, EXPERTS):
            pltpu.make_async_remote_copy(
                src_ref=parts_out.at[block, o], dst_ref=parts_in.at[block, mirrored(o)],
                send_sem=parts_send.at[0], recv_sem=parts_recv.at[block],
                device_id=in_plane(o, section), device_id_type=MESH,
            ).start()

    def first_flat(left, other):
        for block in (left, other):
            others = spread_in.at[block, pl.ds(1, EXPERTS - 1)]
            arrived(others, plane_recv.at[block])
        inputs = jnp.concatenate(
            [spread_in[left].reshape(rows, FLAT), spread_in[other].reshape(rows, FLAT)], axis=0
        )
        total[...] = jnp.dot(inputs, first[:FLAT], preferred_element_type=F32)

    def first_slots(left, other):
        inputs = jnp.concatenate(
            [slots[left].reshape(rows, rest), slots[other].reshape(rows, rest)], axis=0
        )
        value = total[...] + jnp.dot(inputs, first[FLAT:], preferred_element_type=F32)
        hidden[...] = jax.nn.gelu(value, approximate=True).astype(BF16)

    def second_flat(left, other, low, high):
        def tile(t, inner):
            cols = pl.ds(pl.multiple_of(t * BACK_STEP, BACK_STEP), BACK_STEP)
            result = jnp.dot(hidden[...], second[:, cols], preferred_element_type=F32)
            result = result.astype(BF16).reshape(2, EXPERTS, capacity, BACK_STEP)
            parts_out[left, :, :, cols] = result[0]
            parts_out[other, :, :, cols] = result[1]
            parts_in[left, 0, :, cols] = result[0, 0]
            parts_in[other, 0, :, cols] = result[1, 0]
            return inner

        lax.fori_loop(low, high, tile, 0)

    def second_slots(left, other, low, high):
        def tile(t, inner):
            cols = pl.ds(pl.multiple_of(t * SLOT_STEP, SLOT_STEP), SLOT_STEP)
            from_second = pl.ds(pl.multiple_of(BACK + t * SLOT_STEP, SLOT_STEP), SLOT_STEP)
            result = jnp.dot(hidden[...], second[:, from_second], preferred_element_type=F32)
            result = result.reshape(2, EXPERTS, capacity, SLOT_STEP)
            partial[left, :, :, cols] = result[0]
            partial[other, :, :, cols] = result[1]
            return inner

        lax.fori_loop(low, high, tile, 0)

    flat_tiles, slot_tiles = BACK // BACK_STEP, back_rest // SLOT_STEP

    def stage(k, carry):
        left, right = along(RING - (k - 1)), along(k - 1)

        def hop(o, inner):
            ring_slot(k, o)

            @pl.when(o == 0)
            def _():
                first_flat(left, right)

            @pl.when(o == 1)
            def _():
                first_slots(left, right)

            @pl.when((o > 1) & (o < 6))
            def _():
                i = o - 2
                second_flat(left, right, i * flat_tiles // 4, (i + 1) * flat_tiles // 4)
                second_slots(left, right, i * slot_tiles // 4, (i + 1) * slot_tiles // 4)

            return inner

        lax.fori_loop(0, EXPERTS, hop, 0)

        return carry

    lax.fori_loop(2, half, stage, 0)

    def finish(k, carry):
        left, right = along(RING - k), along(k)
        other = jnp.where(k < half, right, z)

        @pl.when(k == half)
        def _():
            def land(o, inner):
                arrived(slots.at[left, o], ring_recv.at[left, o])
                return inner

            lax.fori_loop(0, EXPERTS, land, 0)

        first_flat(left, other)
        first_slots(left, other)
        second_slots(left, other, 0, slot_tiles)

        def early(i, inner):
            pass_on(0, 1, EXPERTS - 1 - 2 * i, False)
            pass_on(1, 1, EXPERTS - 2 - 2 * i, False)
            return inner

        def start(i, inner):
            pass_on(0, 0, EXPERTS - 2 - 2 * i, False)
            pass_on(1, 0, EXPERTS - 1 - 2 * i, False)
            return inner

        @pl.when(k == half - 1)
        def _():
            lax.fori_loop(0, EXPERTS // 2, early, 0)

        @pl.when(k == half)
        def _():
            lax.fori_loop(0, EXPERTS // 2, start, 0)

        second_flat(left, other, 0, flat_tiles)
        give_back(left)

        @pl.when(k == half - 1)
        def _():
            give_back(other)

        return carry

    lax.fori_loop(half - 1, half + 1, finish, 0)
    give_back(along(RING - 2))
    give_back(along(2))
    give_back(along(last))
    give_back(along(1))
    give_back(z)

    def second_hop(i, carry):
        pass_on(0, 1, EXPERTS - 2 - 2 * i, True)
        pass_on(1, 1, EXPERTS - 1 - 2 * i, True)
        return carry

    lax.fori_loop(0, EXPERTS // 2, second_hop, 0)

    def later(j, low, high):
        def one(i, carry):
            pass_on(0, j, EXPERTS - 1 - i, True)
            pass_on(1, j, EXPERTS - 1 - i, True)
            return carry

        lax.fori_loop(low, high, one, 0)

    def later_flat(j):
        def one(c, carry):
            pass_flat(0, j, c, True)
            pass_flat(1, j, c, True)
            return carry

        lax.fori_loop(0, PIECES, one, 0)

    def unpack(block):
        others = parts_in.at[block, pl.ds(1, EXPERTS - 1)]
        arrived(others, parts_recv.at[block])
        picks = routes(block)[:, :rows]
        for c in range(BACK // BACK_STEP):
            cols = slice(c * BACK_STEP, (c + 1) * BACK_STEP)
            source = parts_in[block, :, :, cols].reshape(rows, BACK_STEP)
            value = jnp.dot(picks, source, preferred_element_type=F32)
            whole[block, :, :, cols] = value.reshape(PIECES, piece, BACK_STEP)

    def both(k):
        def one(i, carry):
            unpack(along(jnp.where(i == 0, RING - k, k)))
            return carry

        lax.fori_loop(0, 2, one, 0)

    both(half - 1)
    for c in range(0, PIECES, 2):
        pass_flat(0, 1, c + 1, False)
        pass_flat(1, 1, c, False)
    later(2, 0, EXPERTS)
    unpack(along(half))
    for c in range(0, PIECES, 2):
        pass_flat(0, 0, c, False)
        pass_flat(1, 0, c + 1, False)
    later(3, 0, EXPERTS // 2)
    for c in range(0, PIECES, 2):
        pass_flat(0, 1, c, True)
        pass_flat(1, 1, c + 1, True)
    later(3, EXPERTS // 2, EXPERTS)
    both(2)
    later_flat(2)

    for o in reversed(range(EXPERTS)):
        value = partial[z, o]
        for way in range(2):
            arrived(arriving.at[way, half - 1, o], sum_sem(way, half - 1, o, 0))
            value = value + arriving[way, half - 1, o].astype(F32)
        summed[o] = value.astype(BF16)
        pltpu.make_async_remote_copy(
            src_ref=summed.at[o], dst_ref=returned.at[mirrored(o)],
            send_sem=back_send.at[0], recv_sem=back_recv.at[0],
            device_id=in_plane(o, following), device_id_type=MESH,
        ).start()

    both(1)
    later_flat(3)
    unpack(z)
    for copy in passes:
        copy.wait()
    for c in range(PIECES):
        value = whole[z, c] + act[c * piece:(c + 1) * piece, :BACK].astype(F32)
        for way in range(2):
            arrived(flat_arriving.at[way, half - 1, c], flat_sum_sem(way, half - 1, c))
            value = value + flat_arriving[way, half - 1, c].astype(F32)
        flat_summed[c] = value.astype(BF16)
        pltpu.make_async_remote_copy(
            src_ref=flat_summed.at[c], dst_ref=flat_returned.at[c],
            send_sem=flat_back_send.at[0], recv_sem=flat_back_recv.at[c],
            device_id=(following, me), device_id_type=MESH,
        ).start()

    arrived(returned, back_recv.at[0])
    picks = where_from[:, :rows]
    for c in range(back_rest // SLOT_STEP):
        cols = slice(c * SLOT_STEP, (c + 1) * SLOT_STEP)
        to = slice(BACK + c * SLOT_STEP, BACK + (c + 1) * SLOT_STEP)
        mixed = jnp.dot(picks, returned[:, :, cols].reshape(rows, SLOT_STEP), preferred_element_type=F32)
        out[0, :, to] = (residual[:, cols].astype(F32) + mixed).astype(BF16)
    for c in range(PIECES):
        arrived(flat_returned.at[c], flat_back_recv.at[c])
        out[0, c * piece:(c + 1) * piece, :BACK] = flat_returned[c]

    arrived(packed.at[pl.ds(1, EXPERTS - 1)], give_send.at[0])
    arrived(slots.at[pl.ds(0, RING - 1)], ring_send.at[0])
    arrived(sending.at[pl.ds(0, 2 * half * EXPERTS - EXPERTS)], sum_send.at[0])
    arrived(flat.at[pl.ds(0, RING - 1)], flat_send.at[0])
    arrived(spread_out.at[pl.ds(0, RING - 1)], plane_send.at[0])
    arrived(parts_out.at[pl.ds(0, RING - 1)], parts_send.at[0])
    arrived(flat_sending.at[pl.ds(0, 2 * half * PIECES - PIECES)], flat_sum_send.at[0])
    arrived(summed, back_send.at[0])
    arrived(flat_summed, flat_back_send.at[0])


def per_device(sections, n, activations, norm_gain, in_proj, out_proj, expert_ids):
    tokens, width = activations.shape[1:]
    ff = in_proj.shape[2]
    capacity = 2 * tokens // EXPERTS
    rows = EXPERTS * capacity
    rest, back_rest, piece, half = width - FLAT, width - BACK, tokens // PIECES, RING // 2
    dma = pltpu.SemaphoreType.DMA
    vmem = pltpu.VMEM
    return pl.pallas_call(
        functools.partial(kernel, sections, n, capacity),
        out_shape=pltpu.VMEM(activations.shape, activations.dtype),
        in_specs=[pl.BlockSpec(memory_space=pl.ANY)] * 5,
        out_specs=pl.BlockSpec(memory_space=pltpu.VMEM),
        scratch_shapes=[
            vmem((tokens, width), BF16),
            vmem((1, width), F32),
            vmem((1, tokens), jnp.int32),
            vmem((width, ff), BF16),
            vmem((ff, width), BF16),
            vmem((tokens, rest), BF16),
            vmem((EXPERTS, capacity, rest), BF16),
            vmem((RING, EXPERTS, capacity, rest), BF16),
            vmem((RING, PIECES, piece, FLAT + LANES), BF16),
            vmem((RING, EXPERTS, capacity, FLAT), BF16),
            vmem((RING, EXPERTS, capacity, FLAT), BF16),
            vmem((2 * rows, ff), F32),
            vmem((2 * rows, ff), BF16),
            vmem((RING, EXPERTS, capacity, back_rest), F32),
            vmem((2 * half * EXPERTS, capacity, back_rest), BF16),
            vmem((2, half, EXPERTS, capacity, back_rest), BF16),
            vmem((EXPERTS, capacity, back_rest), BF16),
            vmem((EXPERTS, capacity, back_rest), BF16),
            vmem((RING, EXPERTS, capacity, BACK), BF16),
            vmem((RING, EXPERTS, capacity, BACK), BF16),
            vmem((RING, PIECES, piece, BACK), F32),
            vmem((2 * half * PIECES, piece, BACK), BF16),
            vmem((2, half, PIECES, piece, BACK), BF16),
            vmem((PIECES, piece, BACK), BF16),
            vmem((PIECES, piece, BACK), BF16),
            vmem((tokens, LANES), BF16),
            vmem((tokens, back_rest), BF16),
            vmem((tokens, LANES), BF16),
            dma((3,)),
            dma((2,)),
            dma((2,)),
            dma((2,)),
            dma((1,)),
            dma((1,)),
            dma((RING, EXPERTS)),
            dma((1,)),
            dma((1,)),
            dma((1,)),
            dma((1,)),
            dma((RING, PIECES)),
            dma((1,)),
            dma((RING,)),
            dma((1,)),
            dma((RING,)),
            dma((1,)),
            dma((1,)),
            dma((PIECES,)),
        ],
        compiler_params=pltpu.CompilerParams(
            collective_id=0, has_side_effects=True, vmem_limit_bytes=62 * 1024 * 1024
        ),
    )(activations, norm_gain, expert_ids.reshape(1, tokens), in_proj, out_proj)


def solution(mesh):
    return jax.shard_map(
        functools.partial(per_device, mesh.shape["section"], mesh.shape["expert"]),
        mesh=mesh,
        in_specs=(
            P("section", "expert", None),
            P("section", None),
            P("section", None, "expert"),
            P("section", "expert", None),
            P("section", "expert", None),
        ),
        out_specs=P("section", "expert", None),
        check_vma=False,
    )
```

```python
import functools

import jax
import jax.numpy as jnp
from jax import lax
from jax.experimental import pallas as pl
from jax.experimental.pallas import tpu as pltpu
from jax.sharding import PartitionSpec as P

EXPERTS = 8
RING = 8
NX = 4
FLAT = 2176
BACK = 2048
PIECES = 4
LANES = 128
FIRST_PACK, SLOT_PACK = 2176, 640
BACK_STEP, SLOT_STEP = 2048, 1024
NEAR = ((0, 0), (0, 1), (0, 3), (1, 0), (0, 2), (1, 1), (1, 3), (1, 2))
MESH = pl.DeviceIdType.MESH
F32, BF16 = jnp.float32, jnp.bfloat16

epsilon = 1e-06


def neighbour(group, o):
    dy, dx = NEAR[o]
    return lax.rem(group // NX + dy, EXPERTS // NX) * NX + lax.rem(group % NX + dx, NX)


def mirrored(o):
    dy, dx = NEAR[o]
    return NEAR.index((dy, (NX - dx) % NX))


def placement(routed, ranks, capacity, group, rows):
    row = lax.broadcasted_iota(jnp.int32, (rows, routed.shape[1]), 0)
    place = row // capacity
    owner = jnp.full_like(place, -1)
    for o in range(EXPERTS):
        owner = jnp.where(place == o, neighbour(group, o), owner)
    return jnp.where((owner == routed) & (row % capacity == ranks), 1.0, 0.0).astype(F32)


def arrived(ref, sem):
    pltpu.make_async_copy(ref, ref, sem).wait()


def kernel(
    sections, n, capacity, act_hbm, gain_hbm, ids_hbm, first_hbm, second_hbm, out,
    act, gain, ids, first, second, normed, packed, slots, flat, spread_out, spread_in, total, hidden,
    partial, sending, arriving, summed, returned,
    parts_out, parts_in, whole, flat_sending, flat_arriving, flat_summed, flat_returned,
    where_to, residual, where_from,
    small_sem, weight_sem, pass_send, pass_recv, give_send, ring_send, ring_recv, sum_send, back_send, back_recv,
    flat_send, flat_recv, plane_send, plane_recv, parts_send, parts_recv, flat_sum_send,
    flat_back_send, flat_back_recv, beyond,
):
    section, me = lax.axis_index("section"), lax.axis_index("expert")
    following, leading = lax.rem(section + 1, sections), lax.rem(section + sections - 1, sections)
    group, z = me // RING, lax.rem(me, RING)
    tokens, width = act.shape
    rows = EXPERTS * capacity
    rest, back_rest = width - FLAT, width - BACK
    half = RING // 2
    piece = tokens // PIECES
    last = RING - 1

    def along(k):
        return lax.rem(z + k, RING)

    def on_ring(k):
        return (section, group * RING + along(k))

    def in_plane(o, which):
        return (which, neighbour(group, o) * RING + z)

    smalls = [
        pltpu.make_async_copy(act_hbm.at[0], act, small_sem.at[0]),
        pltpu.make_async_copy(gain_hbm, gain, small_sem.at[1]),
        pltpu.make_async_copy(ids_hbm, ids, small_sem.at[2]),
    ]
    weights = [
        pltpu.make_async_copy(first_hbm.at[0], first, weight_sem.at[0]),
        pltpu.make_async_copy(second_hbm.at[0], second, weight_sem.at[1]),
    ]
    for copy in smalls:
        copy.start()
    barrier = pltpu.get_barrier_semaphore()
    greeted = [in_plane(o, section) for o in range(1, 4)] + [on_ring(1), on_ring(last), in_plane(0, leading)]
    for peer in greeted:
        pl.semaphore_signal(barrier, inc=1, device_id=peer, device_id_type=MESH)
    for copy in smalls:
        copy.wait()
    for copy in weights:
        copy.start()

    floats = act[...].astype(F32)
    scale = lax.rsqrt(jnp.mean(floats * floats, axis=-1, keepdims=True) + epsilon)
    values = (floats * scale * gain[...]).astype(BF16)
    normed[...] = values[:, FLAT:]
    flat[z, :, :, :FLAT] = values[:, :FLAT].reshape(PIECES, piece, FLAT)
    routed = ids[...]
    expert = lax.broadcasted_iota(jnp.int32, (EXPERTS, tokens), 0)
    onehot = jnp.where(expert == routed, 1.0, 0.0).astype(F32)
    earlier = lax.broadcasted_iota(jnp.int32, (tokens, tokens), 0) < lax.broadcasted_iota(
        jnp.int32, (tokens, tokens), 1
    )
    before = jnp.dot(
        onehot.astype(BF16), jnp.where(earlier, 1.0, 0.0).astype(BF16), preferred_element_type=F32
    )
    ranks = jnp.sum(before * onehot, axis=0, keepdims=True).astype(jnp.int32)
    placing = placement(routed, ranks, capacity, group, LANES)
    back = placing.T.astype(BF16)
    where_to[...] = back
    flat[z, :, :, FLAT:] = back.reshape(PIECES, piece, LANES)
    placing = placing[:rows].astype(BF16)

    pl.semaphore_wait(barrier, len(greeted))

    def forward_flat(block, c, k):
        pltpu.make_async_remote_copy(
            src_ref=flat.at[block, c], dst_ref=flat.at[block, c],
            send_sem=flat_send.at[0], recv_sem=flat_recv.at[block, c],
            device_id=on_ring(k), device_id_type=MESH,
        ).start()

    def forward(block, o, k):
        pltpu.make_async_remote_copy(
            src_ref=slots.at[block, o], dst_ref=slots.at[block, o],
            send_sem=ring_send.at[0], recv_sem=ring_recv.at[block, o],
            device_id=on_ring(k), device_id_type=MESH,
        ).start()

    for o in (1, 2):
        pl.semaphore_signal(beyond.at[0], inc=1, device_id=in_plane(o, section), device_id_type=MESH)
    for c in range(PIECES):
        forward_flat(z, c, 1)
        forward_flat(z, c, last)

    for c in range(rest // SLOT_PACK):
        cols = slice(c * SLOT_PACK, (c + 1) * SLOT_PACK)
        block = jnp.dot(placing, normed[:, cols], preferred_element_type=F32)
        packed[:, :, cols] = block.astype(BF16).reshape(EXPERTS, capacity, SLOT_PACK)
    slots[z, 0] = packed[0]

    def give(o):
        pltpu.make_async_remote_copy(
            src_ref=packed.at[o], dst_ref=slots.at[z, mirrored(o)],
            send_sem=give_send.at[0], recv_sem=ring_recv.at[z, mirrored(o)],
            device_id=in_plane(o, section), device_id_type=MESH,
        ).start()

    for o in (1, 2, 3):
        give(o)
    forward(z, 0, 1)
    forward(z, 0, last)
    pl.semaphore_wait(beyond.at[0], 2)
    pl.semaphore_signal(beyond.at[1], inc=1, device_id=in_plane(3, section), device_id_type=MESH)
    for o in (4, 5, 6):
        give(o)

    def routes(block):
        return flat[block, :, :, FLAT:].reshape(tokens, LANES)

    def pack(block, first=False):
        to_slot = routes(block).astype(F32).T[:rows].astype(BF16)
        for c in range(FLAT // FIRST_PACK):
            cols = slice(c * FIRST_PACK, (c + 1) * FIRST_PACK)
            source = flat[block, :, :, cols].reshape(tokens, FIRST_PACK)
            value = jnp.dot(to_slot, source, preferred_element_type=F32)
            value = value.astype(BF16).reshape(EXPERTS, capacity, FIRST_PACK)
            spread_out[block, :, :, cols] = value
            spread_in[block, 0, :, cols] = value[0]
        if first:
            pl.semaphore_wait(beyond.at[1], 1)
            give(7)
        for o in range(1, EXPERTS):
            pltpu.make_async_remote_copy(
                src_ref=spread_out.at[block, o], dst_ref=spread_in.at[block, mirrored(o)],
                send_sem=plane_send.at[0], recv_sem=plane_recv.at[block],
                device_id=in_plane(o, section), device_id_type=MESH,
            ).start()

    pack(z, first=True)
    passes = [
        pltpu.make_async_remote_copy(
            src_ref=src, dst_ref=dst, send_sem=pass_send.at[k], recv_sem=pass_recv.at[k],
            device_id=(following, me), device_id_type=MESH,
        )
        for k, (src, dst) in enumerate(((act.at[:, pl.ds(BACK, back_rest)], residual), (where_to, where_from)))
    ]
    for copy in passes:
        copy.start()

    def spread(o):
        arrived(slots.at[z, o], ring_recv.at[z, o])
        forward(z, o, 1)
        forward(z, o, last)

    def ring_slot(k, o):
        left, right = along(RING - k), along(k)
        arrived(slots.at[left, o], ring_recv.at[left, o])

        @pl.when((k < half - 1) | ((k == half - 1) & (o % 2 == 0)))
        def _():
            forward(left, o, 1)

        @pl.when(k < half)
        def _():
            arrived(slots.at[right, o], ring_recv.at[right, o])

        @pl.when((k < half - 1) | ((k == half - 1) & (o % 2 == 1)))
        def _():
            forward(right, o, last)

    def ring_flat(k, beside):
        left, right = along(RING - k), along(k)

        def hop(c, inner):
            arrived(flat.at[left, c], flat_recv.at[left, c])
            if k < half - 1:
                forward_flat(left, c, 1)
            if k < half:
                arrived(flat.at[right, c], flat_recv.at[right, c])
            if k < half - 1:
                forward_flat(right, c, last)
            if k == half - 1:
                @pl.when(c % 2 == 0)
                def _():
                    forward_flat(left, c, 1)

                @pl.when(c % 2 == 1)
                def _():
                    forward_flat(right, c, last)

            beside(c)
            return inner

        lax.fori_loop(0, PIECES, hop, 0)

        def fill(i, inner):
            pack(along(jnp.where(i == 0, RING - k, k)))
            return inner

        lax.fori_loop(0, 2 if k < half else 1, fill, 0)

    def near(c):
        @pl.when(c > 0)
        def _():
            spread(c)

    ring_flat(1, near)
    ring_flat(2, lambda c: spread(PIECES + c))
    ring_flat(3, lambda c: ring_slot(jnp.int32(1), c))
    ring_flat(4, lambda c: ring_slot(jnp.int32(1), PIECES + c))
    for copy in weights:
        copy.wait()

    def sum_sem(way, j, o, shift):
        return ring_recv.at[along((j + shift) if way == 0 else (2 * RING - j - shift)), o]

    def flat_sum_sem(way, j, c):
        return flat_recv.at[way * half + j, c]

    def pass_on(way, j, o, add):
        distance = half - j
        block = along(distance if way == 0 else RING - distance)
        value = partial[block, o]
        if add:
            arrived(arriving.at[way, j - 1, o], sum_sem(way, j - 1, o, 0))
            value = value + arriving[way, j - 1, o].astype(F32)
        place = (way * half + j) * EXPERTS + o
        sending[place] = value.astype(BF16)
        pltpu.make_async_remote_copy(
            src_ref=sending.at[place], dst_ref=arriving.at[way, j, o],
            send_sem=sum_send.at[0], recv_sem=sum_sem(way, j, o, 1),
            device_id=on_ring(1 if way == 0 else last), device_id_type=MESH,
        ).start()

    def pass_flat(way, j, c, add):
        distance = half - j
        block = along(distance if way == 0 else RING - distance)
        value = whole[block, c]
        if add:
            arrived(flat_arriving.at[way, j - 1, c], flat_sum_sem(way, j - 1, c))
            value = value + flat_arriving[way, j - 1, c].astype(F32)
        place = (way * half + j) * PIECES + c
        flat_sending[place] = value.astype(BF16)
        pltpu.make_async_remote_copy(
            src_ref=flat_sending.at[place], dst_ref=flat_arriving.at[way, j, c],
            send_sem=flat_sum_send.at[0], recv_sem=flat_sum_sem(way, j, c),
            device_id=on_ring(1 if way == 0 else last), device_id_type=MESH,
        ).start()

    def give_back(block):
        for o in range(1, EXPERTS):
            pltpu.make_async_remote_copy(
                src_ref=parts_out.at[block, o], dst_ref=parts_in.at[block, mirrored(o)],
                send_sem=parts_send.at[0], recv_sem=parts_recv.at[block],
                device_id=in_plane(o, section), device_id_type=MESH,
            ).start()

    def first_flat(left, other):
        for block in (left, other):
            others = spread_in.at[block, pl.ds(1, EXPERTS - 1)]
            arrived(others, plane_recv.at[block])
        inputs = jnp.concatenate(
            [spread_in[left].reshape(rows, FLAT), spread_in[other].reshape(rows, FLAT)], axis=0
        )
        total[...] = jnp.dot(inputs, first[:FLAT], preferred_element_type=F32)

    def first_slots(left, other):
        inputs = jnp.concatenate(
            [slots[left].reshape(rows, rest), slots[other].reshape(rows, rest)], axis=0
        )
        value = total[...] + jnp.dot(inputs, first[FLAT:], preferred_element_type=F32)
        hidden[...] = jax.nn.gelu(value, approximate=True).astype(BF16)

    def second_flat(left, other, low, high):
        def tile(t, inner):
            cols = pl.ds(pl.multiple_of(t * BACK_STEP, BACK_STEP), BACK_STEP)
            result = jnp.dot(hidden[...], second[:, cols], preferred_element_type=F32)
            result = result.astype(BF16).reshape(2, EXPERTS, capacity, BACK_STEP)
            parts_out[left, :, :, cols] = result[0]
            parts_out[other, :, :, cols] = result[1]
            parts_in[left, 0, :, cols] = result[0, 0]
            parts_in[other, 0, :, cols] = result[1, 0]
            return inner

        lax.fori_loop(low, high, tile, 0)

    def second_slots(left, other, low, high):
        def tile(t, inner):
            cols = pl.ds(pl.multiple_of(t * SLOT_STEP, SLOT_STEP), SLOT_STEP)
            from_second = pl.ds(pl.multiple_of(BACK + t * SLOT_STEP, SLOT_STEP), SLOT_STEP)
            result = jnp.dot(hidden[...], second[:, from_second], preferred_element_type=F32)
            result = result.reshape(2, EXPERTS, capacity, SLOT_STEP)
            partial[left, :, :, cols] = result[0]
            partial[other, :, :, cols] = result[1]
            return inner

        lax.fori_loop(low, high, tile, 0)

    flat_tiles, slot_tiles = BACK // BACK_STEP, back_rest // SLOT_STEP

    def stage(k, carry):
        left, right = along(RING - (k - 1)), along(k - 1)

        def hop(o, inner):
            ring_slot(k, o)

            @pl.when(o == 0)
            def _():
                first_flat(left, right)

            @pl.when(o == 1)
            def _():
                first_slots(left, right)

            @pl.when((o > 1) & (o < 6))
            def _():
                i = o - 2
                second_flat(left, right, i * flat_tiles // 4, (i + 1) * flat_tiles // 4)
                second_slots(left, right, i * slot_tiles // 4, (i + 1) * slot_tiles // 4)

            return inner

        lax.fori_loop(0, EXPERTS, hop, 0)

        return carry

    lax.fori_loop(2, half, stage, 0)

    def finish(k, carry):
        left, right = along(RING - k), along(k)
        other = jnp.where(k < half, right, z)

        @pl.when(k == half)
        def _():
            def land(o, inner):
                arrived(slots.at[left, o], ring_recv.at[left, o])
                return inner

            lax.fori_loop(0, EXPERTS, land, 0)

        first_flat(left, other)
        first_slots(left, other)
        second_slots(left, other, 0, slot_tiles)

        def early(i, inner):
            pass_on(0, 1, EXPERTS - 1 - 2 * i, False)
            pass_on(1, 1, EXPERTS - 2 - 2 * i, False)
            return inner

        def start(i, inner):
            pass_on(0, 0, EXPERTS - 2 - 2 * i, False)
            pass_on(1, 0, EXPERTS - 1 - 2 * i, False)
            return inner

        @pl.when(k == half - 1)
        def _():
            lax.fori_loop(0, EXPERTS // 2, early, 0)

        @pl.when(k == half)
        def _():
            lax.fori_loop(0, EXPERTS // 2, start, 0)

        second_flat(left, other, 0, flat_tiles)
        give_back(left)

        @pl.when(k == half - 1)
        def _():
            give_back(other)

        return carry

    lax.fori_loop(half - 1, half + 1, finish, 0)
    give_back(along(RING - 2))
    give_back(along(2))
    give_back(along(last))
    give_back(along(1))
    give_back(z)

    def second_hop(i, carry):
        pass_on(0, 1, EXPERTS - 2 - 2 * i, True)
        pass_on(1, 1, EXPERTS - 1 - 2 * i, True)
        return carry

    lax.fori_loop(0, EXPERTS // 2, second_hop, 0)

    def later(j, low, high):
        def one(i, carry):
            pass_on(0, j, EXPERTS - 1 - i, True)
            pass_on(1, j, EXPERTS - 1 - i, True)
            return carry

        lax.fori_loop(low, high, one, 0)

    def later_flat(j):
        def one(c, carry):
            pass_flat(0, j, c, True)
            pass_flat(1, j, c, True)
            return carry

        lax.fori_loop(0, PIECES, one, 0)

    def unpack(block):
        others = parts_in.at[block, pl.ds(1, EXPERTS - 1)]
        arrived(others, parts_recv.at[block])
        picks = routes(block)[:, :rows]
        for c in range(BACK // BACK_STEP):
            cols = slice(c * BACK_STEP, (c + 1) * BACK_STEP)
            source = parts_in[block, :, :, cols].reshape(rows, BACK_STEP)
            value = jnp.dot(picks, source, preferred_element_type=F32)
            whole[block, :, :, cols] = value.reshape(PIECES, piece, BACK_STEP)

    def both(k):
        def one(i, carry):
            unpack(along(jnp.where(i == 0, RING - k, k)))
            return carry

        lax.fori_loop(0, 2, one, 0)

    both(half - 1)
    for c in range(0, PIECES, 2):
        pass_flat(0, 1, c + 1, False)
        pass_flat(1, 1, c, False)
    later(2, 0, EXPERTS)
    unpack(along(half))
    for c in range(0, PIECES, 2):
        pass_flat(0, 0, c, False)
        pass_flat(1, 0, c + 1, False)
    later(3, 0, EXPERTS // 2)
    for c in range(0, PIECES, 2):
        pass_flat(0, 1, c, True)
        pass_flat(1, 1, c + 1, True)
    later(3, EXPERTS // 2, EXPERTS)
    both(2)
    later_flat(2)

    for o in reversed(range(EXPERTS)):
        value = partial[z, o]
        for way in range(2):
            arrived(arriving.at[way, half - 1, o], sum_sem(way, half - 1, o, 0))
            value = value + arriving[way, half - 1, o].astype(F32)
        summed[o] = value.astype(BF16)
        pltpu.make_async_remote_copy(
            src_ref=summed.at[o], dst_ref=returned.at[mirrored(o)],
            send_sem=back_send.at[0], recv_sem=back_recv.at[0],
            device_id=in_plane(o, following), device_id_type=MESH,
        ).start()

    both(1)
    later_flat(3)
    unpack(z)
    for copy in passes:
        copy.wait()
    for c in range(PIECES):
        value = whole[z, c] + act[c * piece:(c + 1) * piece, :BACK].astype(F32)
        for way in range(2):
            arrived(flat_arriving.at[way, half - 1, c], flat_sum_sem(way, half - 1, c))
            value = value + flat_arriving[way, half - 1, c].astype(F32)
        flat_summed[c] = value.astype(BF16)
        pltpu.make_async_remote_copy(
            src_ref=flat_summed.at[c], dst_ref=flat_returned.at[c],
            send_sem=flat_back_send.at[0], recv_sem=flat_back_recv.at[c],
            device_id=(following, me), device_id_type=MESH,
        ).start()

    arrived(returned, back_recv.at[0])
    picks = where_from[:, :rows]
    for c in range(back_rest // SLOT_STEP):
        cols = slice(c * SLOT_STEP, (c + 1) * SLOT_STEP)
        to = slice(BACK + c * SLOT_STEP, BACK + (c + 1) * SLOT_STEP)
        mixed = jnp.dot(picks, returned[:, :, cols].reshape(rows, SLOT_STEP), preferred_element_type=F32)
        out[0, :, to] = (residual[:, cols].astype(F32) + mixed).astype(BF16)
    for c in range(PIECES):
        arrived(flat_returned.at[c], flat_back_recv.at[c])
        out[0, c * piece:(c + 1) * piece, :BACK] = flat_returned[c]

    arrived(packed.at[pl.ds(1, EXPERTS - 1)], give_send.at[0])
    arrived(slots.at[pl.ds(0, RING - 1)], ring_send.at[0])
    arrived(sending.at[pl.ds(0, 2 * half * EXPERTS - EXPERTS)], sum_send.at[0])
    arrived(flat.at[pl.ds(0, RING - 1)], flat_send.at[0])
    arrived(spread_out.at[pl.ds(0, RING - 1)], plane_send.at[0])
    arrived(parts_out.at[pl.ds(0, RING - 1)], parts_send.at[0])
    arrived(flat_sending.at[pl.ds(0, 2 * half * PIECES - PIECES)], flat_sum_send.at[0])
    arrived(summed, back_send.at[0])
    arrived(flat_summed, flat_back_send.at[0])


def per_device(sections, n, activations, norm_gain, in_proj, out_proj, expert_ids):
    tokens, width = activations.shape[1:]
    ff = in_proj.shape[2]
    capacity = 2 * tokens // EXPERTS
    rows = EXPERTS * capacity
    rest, back_rest, piece, half = width - FLAT, width - BACK, tokens // PIECES, RING // 2
    dma = pltpu.SemaphoreType.DMA
    vmem = pltpu.VMEM
    return pl.pallas_call(
        functools.partial(kernel, sections, n, capacity),
        out_shape=pltpu.VMEM(activations.shape, activations.dtype),
        in_specs=[pl.BlockSpec(memory_space=pl.ANY)] * 5,
        out_specs=pl.BlockSpec(memory_space=pltpu.VMEM),
        scratch_shapes=[
            vmem((tokens, width), BF16),
            vmem((1, width), F32),
            vmem((1, tokens), jnp.int32),
            vmem((width, ff), BF16),
            vmem((ff, width), BF16),
            vmem((tokens, rest), BF16),
            vmem((EXPERTS, capacity, rest), BF16),
            vmem((RING, EXPERTS, capacity, rest), BF16),
            vmem((RING, PIECES, piece, FLAT + LANES), BF16),
            vmem((RING, EXPERTS, capacity, FLAT), BF16),
            vmem((RING, EXPERTS, capacity, FLAT), BF16),
            vmem((2 * rows, ff), F32),
            vmem((2 * rows, ff), BF16),
            vmem((RING, EXPERTS, capacity, back_rest), F32),
            vmem((2 * half * EXPERTS, capacity, back_rest), BF16),
            vmem((2, half, EXPERTS, capacity, back_rest), BF16),
            vmem((EXPERTS, capacity, back_rest), BF16),
            vmem((EXPERTS, capacity, back_rest), BF16),
            vmem((RING, EXPERTS, capacity, BACK), BF16),
            vmem((RING, EXPERTS, capacity, BACK), BF16),
            vmem((RING, PIECES, piece, BACK), F32),
            vmem((2 * half * PIECES, piece, BACK), BF16),
            vmem((2, half, PIECES, piece, BACK), BF16),
            vmem((PIECES, piece, BACK), BF16),
            vmem((PIECES, piece, BACK), BF16),
            vmem((tokens, LANES), BF16),
            vmem((tokens, back_rest), BF16),
            vmem((tokens, LANES), BF16),
            dma((3,)),
            dma((2,)),
            dma((2,)),
            dma((2,)),
            dma((1,)),
            dma((1,)),
            dma((RING, EXPERTS)),
            dma((1,)),
            dma((1,)),
            dma((1,)),
            dma((1,)),
            dma((RING, PIECES)),
            dma((1,)),
            dma((RING,)),
            dma((1,)),
            dma((RING,)),
            dma((1,)),
            dma((1,)),
            dma((PIECES,)),
            pltpu.SemaphoreType.REGULAR((2,)),
        ],
        compiler_params=pltpu.CompilerParams(
            collective_id=0, has_side_effects=True, vmem_limit_bytes=62 * 1024 * 1024
        ),
    )(activations, norm_gain, expert_ids.reshape(1, tokens), in_proj, out_proj)


def solution(mesh):
    return jax.shard_map(
        functools.partial(per_device, mesh.shape["section"], mesh.shape["expert"]),
        mesh=mesh,
        in_specs=(
            P("section", "expert", None),
            P("section", None),
            P("section", None, "expert"),
            P("section", "expert", None),
            P("section", "expert", None),
        ),
        out_specs=P("section", "expert", None),
        check_vma=False,
    )
```

```python
import functools

import jax
import jax.numpy as jnp
from jax import lax
from jax.experimental import pallas as pl
from jax.experimental.pallas import tpu as pltpu
from jax.sharding import PartitionSpec as P

EXPERTS = 8
RING = 8
NX = 4
FLAT = 2176
BACK = 2048
PIECES = 4
LANES = 128
FIRST_PACK, SLOT_PACK = 2176, 640
BACK_STEP, SLOT_STEP = 2048, 1024
NEAR = ((0, 0), (0, 1), (0, 3), (1, 0), (0, 2), (1, 1), (1, 3), (1, 2))
MESH = pl.DeviceIdType.MESH
F32, BF16 = jnp.float32, jnp.bfloat16

epsilon = 1e-06


def neighbour(group, o):
    dy, dx = NEAR[o]
    return lax.rem(group // NX + dy, EXPERTS // NX) * NX + lax.rem(group % NX + dx, NX)


def mirrored(o):
    dy, dx = NEAR[o]
    return NEAR.index((dy, (NX - dx) % NX))


def placement(routed, ranks, capacity, group, rows):
    row = lax.broadcasted_iota(jnp.int32, (rows, routed.shape[1]), 0)
    place = row // capacity
    owner = jnp.full_like(place, -1)
    for o in range(EXPERTS):
        owner = jnp.where(place == o, neighbour(group, o), owner)
    return jnp.where((owner == routed) & (row % capacity == ranks), 1.0, 0.0).astype(F32)


def arrived(ref, sem):
    pltpu.make_async_copy(ref, ref, sem).wait()


def kernel(
    sections, n, capacity, act_hbm, gain_hbm, ids_hbm, first_hbm, second_hbm, out,
    act, gain, ids, first, second, normed, packed, slots, flat, spread_out, spread_in, total, hidden,
    partial, sending, arriving, summed, returned,
    parts_out, parts_in, whole, flat_sending, flat_arriving, flat_summed, flat_returned,
    where_to, residual, where_from,
    small_sem, weight_sem, pass_send, pass_recv, give_send, ring_send, ring_recv, sum_send, back_send, back_recv,
    flat_send, flat_recv, plane_send, plane_recv, parts_send, parts_recv, flat_sum_send,
    flat_back_send, flat_back_recv, beyond,
):
    section, me = lax.axis_index("section"), lax.axis_index("expert")
    following, leading = lax.rem(section + 1, sections), lax.rem(section + sections - 1, sections)
    group, z = me // RING, lax.rem(me, RING)
    tokens, width = act.shape
    rows = EXPERTS * capacity
    rest, back_rest = width - FLAT, width - BACK
    half = RING // 2
    piece = tokens // PIECES
    last = RING - 1

    def along(k):
        return lax.rem(z + k, RING)

    def on_ring(k):
        return (section, group * RING + along(k))

    def in_plane(o, which):
        return (which, neighbour(group, o) * RING + z)

    smalls = [
        pltpu.make_async_copy(act_hbm.at[0], act, small_sem.at[0]),
        pltpu.make_async_copy(gain_hbm, gain, small_sem.at[1]),
        pltpu.make_async_copy(ids_hbm, ids, small_sem.at[2]),
    ]
    weights = [
        pltpu.make_async_copy(first_hbm.at[0], first, weight_sem.at[0]),
        pltpu.make_async_copy(second_hbm.at[0], second, weight_sem.at[1]),
    ]
    for copy in smalls:
        copy.start()
    barrier = pltpu.get_barrier_semaphore()
    greeted = [in_plane(o, section) for o in range(1, 4)] + [on_ring(1), on_ring(last), in_plane(0, leading)]
    for peer in greeted:
        pl.semaphore_signal(barrier, inc=1, device_id=peer, device_id_type=MESH)
    for copy in smalls:
        copy.wait()
    for copy in weights:
        copy.start()

    floats = act[...].astype(F32)
    scale = lax.rsqrt(jnp.mean(floats * floats, axis=-1, keepdims=True) + epsilon)
    values = (floats * scale * gain[...]).astype(BF16)
    normed[...] = values[:, FLAT:]
    flat[z, :, :, :FLAT] = values[:, :FLAT].reshape(PIECES, piece, FLAT)
    routed = ids[...]
    expert = lax.broadcasted_iota(jnp.int32, (EXPERTS, tokens), 0)
    onehot = jnp.where(expert == routed, 1.0, 0.0).astype(F32)
    earlier = lax.broadcasted_iota(jnp.int32, (tokens, tokens), 0) < lax.broadcasted_iota(
        jnp.int32, (tokens, tokens), 1
    )
    before = jnp.dot(
        onehot.astype(BF16), jnp.where(earlier, 1.0, 0.0).astype(BF16), preferred_element_type=F32
    )
    ranks = jnp.sum(before * onehot, axis=0, keepdims=True).astype(jnp.int32)
    placing = placement(routed, ranks, capacity, group, LANES)
    back = placing.T.astype(BF16)
    where_to[...] = back
    flat[z, :, :, FLAT:] = back.reshape(PIECES, piece, LANES)
    placing = placing[:rows].astype(BF16)

    pl.semaphore_wait(barrier, len(greeted))

    def forward_flat(block, c, k):
        pltpu.make_async_remote_copy(
            src_ref=flat.at[block, c], dst_ref=flat.at[block, c],
            send_sem=flat_send.at[0], recv_sem=flat_recv.at[block, c],
            device_id=on_ring(k), device_id_type=MESH,
        ).start()

    def forward(block, o, k):
        pltpu.make_async_remote_copy(
            src_ref=slots.at[block, o], dst_ref=slots.at[block, o],
            send_sem=ring_send.at[0], recv_sem=ring_recv.at[block, o],
            device_id=on_ring(k), device_id_type=MESH,
        ).start()

    for o in (1, 2):
        pl.semaphore_signal(beyond.at[0], inc=1, device_id=in_plane(o, section), device_id_type=MESH)
    for c in range(PIECES):
        forward_flat(z, c, 1)
        forward_flat(z, c, last)

    for c in range(rest // SLOT_PACK):
        cols = slice(c * SLOT_PACK, (c + 1) * SLOT_PACK)
        block = jnp.dot(placing, normed[:, cols], preferred_element_type=F32)
        packed[:, :, cols] = block.astype(BF16).reshape(EXPERTS, capacity, SLOT_PACK)
    slots[z, 0] = packed[0]

    def give(o):
        pltpu.make_async_remote_copy(
            src_ref=packed.at[o], dst_ref=slots.at[z, mirrored(o)],
            send_sem=give_send.at[0], recv_sem=ring_recv.at[z, mirrored(o)],
            device_id=in_plane(o, section), device_id_type=MESH,
        ).start()

    for o in (1, 2, 3):
        give(o)
    forward(z, 0, 1)
    forward(z, 0, last)
    pl.semaphore_wait(beyond.at[0], 2)
    pl.semaphore_signal(beyond.at[1], inc=1, device_id=in_plane(3, section), device_id_type=MESH)
    for o in (4, 5, 6):
        give(o)

    def routes(block):
        return flat[block, :, :, FLAT:].reshape(tokens, LANES)

    def pack(block, first=False):
        to_slot = routes(block).astype(F32).T[:rows].astype(BF16)
        for c in range(FLAT // FIRST_PACK):
            cols = slice(c * FIRST_PACK, (c + 1) * FIRST_PACK)
            source = flat[block, :, :, cols].reshape(tokens, FIRST_PACK)
            value = jnp.dot(to_slot, source, preferred_element_type=F32)
            value = value.astype(BF16).reshape(EXPERTS, capacity, FIRST_PACK)
            spread_out[block, :, :, cols] = value
            spread_in[block, 0, :, cols] = value[0]
        if first:
            pl.semaphore_wait(beyond.at[1], 1)
            give(7)
        for o in range(1, EXPERTS):
            pltpu.make_async_remote_copy(
                src_ref=spread_out.at[block, o], dst_ref=spread_in.at[block, mirrored(o)],
                send_sem=plane_send.at[0], recv_sem=plane_recv.at[block],
                device_id=in_plane(o, section), device_id_type=MESH,
            ).start()

    pack(z, first=True)
    passes = [
        pltpu.make_async_remote_copy(
            src_ref=src, dst_ref=dst, send_sem=pass_send.at[k], recv_sem=pass_recv.at[k],
            device_id=(following, me), device_id_type=MESH,
        )
        for k, (src, dst) in enumerate(((act.at[:, pl.ds(BACK, back_rest)], residual), (where_to, where_from)))
    ]
    for copy in passes:
        copy.start()

    def spread(o):
        arrived(slots.at[z, o], ring_recv.at[z, o])
        forward(z, o, 1)
        forward(z, o, last)

    def ring_slot(k, o):
        left, right = along(RING - k), along(k)
        arrived(slots.at[left, o], ring_recv.at[left, o])

        @pl.when((k < half - 1) | ((k == half - 1) & (o % 2 == 0)))
        def _():
            forward(left, o, 1)

        @pl.when(k < half)
        def _():
            arrived(slots.at[right, o], ring_recv.at[right, o])

        @pl.when((k < half - 1) | ((k == half - 1) & (o % 2 == 1)))
        def _():
            forward(right, o, last)

    def ring_flat(k, beside):
        left, right = along(RING - k), along(k)

        def hop(c, inner):
            arrived(flat.at[left, c], flat_recv.at[left, c])
            if k < half - 1:
                forward_flat(left, c, 1)
            if k < half:
                arrived(flat.at[right, c], flat_recv.at[right, c])
            if k < half - 1:
                forward_flat(right, c, last)
            if k == half - 1:
                @pl.when(c % 2 == 0)
                def _():
                    forward_flat(left, c, 1)

                @pl.when(c % 2 == 1)
                def _():
                    forward_flat(right, c, last)

            beside(c)
            return inner

        lax.fori_loop(0, PIECES, hop, 0)

        def fill(i, inner):
            pack(along(jnp.where(i == 0, RING - k, k)))
            return inner

        lax.fori_loop(0, 2 if k < half else 1, fill, 0)

    def near(c):
        @pl.when(c > 0)
        def _():
            spread(c)

    ring_flat(1, near)
    ring_flat(2, lambda c: spread(PIECES + c))
    ring_flat(3, lambda c: ring_slot(jnp.int32(1), c))
    ring_flat(4, lambda c: ring_slot(jnp.int32(1), PIECES + c))
    for copy in weights:
        copy.wait()

    def sum_sem(way, j, o, shift):
        return ring_recv.at[along((j + shift) if way == 0 else (2 * RING - j - shift)), o]

    def flat_sum_sem(way, j, c):
        return flat_recv.at[way * half + j, c]

    def pass_on(way, j, o, add):
        distance = half - j
        block = along(distance if way == 0 else RING - distance)
        value = partial[block, o]
        if add:
            arrived(arriving.at[way, j - 1, o], sum_sem(way, j - 1, o, 0))
            value = value + arriving[way, j - 1, o].astype(F32)
        place = (way * half + j) * EXPERTS + o
        sending[place] = value.astype(BF16)
        pltpu.make_async_remote_copy(
            src_ref=sending.at[place], dst_ref=arriving.at[way, j, o],
            send_sem=sum_send.at[0], recv_sem=sum_sem(way, j, o, 1),
            device_id=on_ring(1 if way == 0 else last), device_id_type=MESH,
        ).start()

    def pass_flat(way, j, c, add):
        distance = half - j
        block = along(distance if way == 0 else RING - distance)
        value = whole[block, c]
        if add:
            arrived(flat_arriving.at[way, j - 1, c], flat_sum_sem(way, j - 1, c))
            value = value + flat_arriving[way, j - 1, c].astype(F32)
        place = (way * half + j) * PIECES + c
        flat_sending[place] = value.astype(BF16)
        pltpu.make_async_remote_copy(
            src_ref=flat_sending.at[place], dst_ref=flat_arriving.at[way, j, c],
            send_sem=flat_sum_send.at[0], recv_sem=flat_sum_sem(way, j, c),
            device_id=on_ring(1 if way == 0 else last), device_id_type=MESH,
        ).start()

    def give_back(block):
        for o in range(1, EXPERTS):
            pltpu.make_async_remote_copy(
                src_ref=parts_out.at[block, o], dst_ref=parts_in.at[block, mirrored(o)],
                send_sem=parts_send.at[0], recv_sem=parts_recv.at[block],
                device_id=in_plane(o, section), device_id_type=MESH,
            ).start()

    def first_flat(left, other):
        for block in (left, other):
            others = spread_in.at[block, pl.ds(1, EXPERTS - 1)]
            arrived(others, plane_recv.at[block])
        inputs = jnp.concatenate(
            [spread_in[left].reshape(rows, FLAT), spread_in[other].reshape(rows, FLAT)], axis=0
        )
        total[...] = jnp.dot(inputs, first[:FLAT], preferred_element_type=F32)

    def first_slots(left, other):
        inputs = jnp.concatenate(
            [slots[left].reshape(rows, rest), slots[other].reshape(rows, rest)], axis=0
        )
        value = total[...] + jnp.dot(inputs, first[FLAT:], preferred_element_type=F32)
        hidden[...] = jax.nn.gelu(value, approximate=True).astype(BF16)

    def second_flat(left, other, low, high):
        def tile(t, inner):
            cols = pl.ds(pl.multiple_of(t * BACK_STEP, BACK_STEP), BACK_STEP)
            result = jnp.dot(hidden[...], second[:, cols], preferred_element_type=F32)
            result = result.astype(BF16).reshape(2, EXPERTS, capacity, BACK_STEP)
            parts_out[left, :, :, cols] = result[0]
            parts_out[other, :, :, cols] = result[1]
            parts_in[left, 0, :, cols] = result[0, 0]
            parts_in[other, 0, :, cols] = result[1, 0]
            return inner

        lax.fori_loop(low, high, tile, 0)

    def second_slots(left, other, low, high):
        def tile(t, inner):
            cols = pl.ds(pl.multiple_of(t * SLOT_STEP, SLOT_STEP), SLOT_STEP)
            from_second = pl.ds(pl.multiple_of(BACK + t * SLOT_STEP, SLOT_STEP), SLOT_STEP)
            result = jnp.dot(hidden[...], second[:, from_second], preferred_element_type=F32)
            result = result.reshape(2, EXPERTS, capacity, SLOT_STEP)
            partial[left, :, :, cols] = result[0]
            partial[other, :, :, cols] = result[1]
            return inner

        lax.fori_loop(low, high, tile, 0)

    flat_tiles, slot_tiles = BACK // BACK_STEP, back_rest // SLOT_STEP

    def stage(k, carry):
        left, right = along(RING - (k - 1)), along(k - 1)

        def hop(o, inner):
            ring_slot(k, o)

            @pl.when(o == 0)
            def _():
                first_flat(left, right)

            @pl.when(o == 1)
            def _():
                first_slots(left, right)

            @pl.when((o > 1) & (o < 6))
            def _():
                i = o - 2
                second_flat(left, right, i * flat_tiles // 4, (i + 1) * flat_tiles // 4)
                second_slots(left, right, i * slot_tiles // 4, (i + 1) * slot_tiles // 4)

            return inner

        lax.fori_loop(0, EXPERTS, hop, 0)

        return carry

    lax.fori_loop(2, half, stage, 0)

    def finish(k, carry):
        left, right = along(RING - k), along(k)
        other = jnp.where(k < half, right, z)

        @pl.when(k == half)
        def _():
            def land(o, inner):
                arrived(slots.at[left, o], ring_recv.at[left, o])
                return inner

            lax.fori_loop(0, EXPERTS, land, 0)

        first_flat(left, other)
        first_slots(left, other)
        second_slots(left, other, 0, slot_tiles)

        def early(i, inner):
            pass_on(0, 1, EXPERTS - 1 - 2 * i, False)
            pass_on(1, 1, EXPERTS - 2 - 2 * i, False)
            return inner

        def start(i, inner):
            pass_on(0, 0, EXPERTS - 2 - 2 * i, False)
            pass_on(1, 0, EXPERTS - 1 - 2 * i, False)
            return inner

        @pl.when(k == half - 1)
        def _():
            lax.fori_loop(0, EXPERTS // 2, early, 0)

        @pl.when(k == half)
        def _():
            lax.fori_loop(0, EXPERTS // 2, start, 0)

        second_flat(left, other, 0, flat_tiles)
        give_back(left)

        @pl.when(k == half - 1)
        def _():
            give_back(other)

        return carry

    lax.fori_loop(half - 1, half + 1, finish, 0)
    give_back(along(RING - 2))
    give_back(along(2))
    give_back(along(last))
    give_back(along(1))
    give_back(z)

    def second_hop(i, carry):
        pass_on(0, 1, EXPERTS - 2 - 2 * i, True)
        pass_on(1, 1, EXPERTS - 1 - 2 * i, True)
        return carry

    lax.fori_loop(0, EXPERTS // 2, second_hop, 0)

    def later(j, low, high):
        def one(i, carry):
            pass_on(0, j, EXPERTS - 1 - i, True)
            pass_on(1, j, EXPERTS - 1 - i, True)
            return carry

        lax.fori_loop(low, high, one, 0)

    def later_flat(j):
        def one(c, carry):
            pass_flat(0, j, c, True)
            pass_flat(1, j, c, True)
            return carry

        lax.fori_loop(0, PIECES, one, 0)

    def unpack(block):
        others = parts_in.at[block, pl.ds(1, EXPERTS - 1)]
        arrived(others, parts_recv.at[block])
        picks = routes(block)[:, :rows]
        for c in range(BACK // BACK_STEP):
            cols = slice(c * BACK_STEP, (c + 1) * BACK_STEP)
            source = parts_in[block, :, :, cols].reshape(rows, BACK_STEP)
            value = jnp.dot(picks, source, preferred_element_type=F32)
            whole[block, :, :, cols] = value.reshape(PIECES, piece, BACK_STEP)

    def both(k):
        def one(i, carry):
            unpack(along(jnp.where(i == 0, RING - k, k)))
            return carry

        lax.fori_loop(0, 2, one, 0)

    later(2, 0, EXPERTS)
    unpack(along(half))
    for c in range(0, PIECES, 2):
        pass_flat(0, 0, c, False)
        pass_flat(1, 0, c + 1, False)
    both(half - 1)
    for c in range(0, PIECES, 2):
        pass_flat(0, 1, c + 1, False)
        pass_flat(1, 1, c, False)
    later(3, 0, EXPERTS // 2)
    for c in range(0, PIECES, 2):
        pass_flat(0, 1, c, True)
        pass_flat(1, 1, c + 1, True)
    later(3, EXPERTS // 2, EXPERTS)
    both(2)
    later_flat(2)

    for o in reversed(range(EXPERTS)):
        value = partial[z, o]
        for way in range(2):
            arrived(arriving.at[way, half - 1, o], sum_sem(way, half - 1, o, 0))
            value = value + arriving[way, half - 1, o].astype(F32)
        summed[o] = value.astype(BF16)
        pltpu.make_async_remote_copy(
            src_ref=summed.at[o], dst_ref=returned.at[mirrored(o)],
            send_sem=back_send.at[0], recv_sem=back_recv.at[0],
            device_id=in_plane(o, following), device_id_type=MESH,
        ).start()

    both(1)
    later_flat(3)
    unpack(z)
    for copy in passes:
        copy.wait()
    for c in range(PIECES):
        value = whole[z, c] + act[c * piece:(c + 1) * piece, :BACK].astype(F32)
        for way in range(2):
            arrived(flat_arriving.at[way, half - 1, c], flat_sum_sem(way, half - 1, c))
            value = value + flat_arriving[way, half - 1, c].astype(F32)
        flat_summed[c] = value.astype(BF16)
        pltpu.make_async_remote_copy(
            src_ref=flat_summed.at[c], dst_ref=flat_returned.at[c],
            send_sem=flat_back_send.at[0], recv_sem=flat_back_recv.at[c],
            device_id=(following, me), device_id_type=MESH,
        ).start()

    arrived(returned, back_recv.at[0])
    picks = where_from[:, :rows]
    for c in range(back_rest // SLOT_STEP):
        cols = slice(c * SLOT_STEP, (c + 1) * SLOT_STEP)
        to = slice(BACK + c * SLOT_STEP, BACK + (c + 1) * SLOT_STEP)
        mixed = jnp.dot(picks, returned[:, :, cols].reshape(rows, SLOT_STEP), preferred_element_type=F32)
        out[0, :, to] = (residual[:, cols].astype(F32) + mixed).astype(BF16)
    for c in range(PIECES):
        arrived(flat_returned.at[c], flat_back_recv.at[c])
        out[0, c * piece:(c + 1) * piece, :BACK] = flat_returned[c]

    arrived(packed.at[pl.ds(1, EXPERTS - 1)], give_send.at[0])
    arrived(slots.at[pl.ds(0, RING - 1)], ring_send.at[0])
    arrived(sending.at[pl.ds(0, 2 * half * EXPERTS - EXPERTS)], sum_send.at[0])
    arrived(flat.at[pl.ds(0, RING - 1)], flat_send.at[0])
    arrived(spread_out.at[pl.ds(0, RING - 1)], plane_send.at[0])
    arrived(parts_out.at[pl.ds(0, RING - 1)], parts_send.at[0])
    arrived(flat_sending.at[pl.ds(0, 2 * half * PIECES - PIECES)], flat_sum_send.at[0])
    arrived(summed, back_send.at[0])
    arrived(flat_summed, flat_back_send.at[0])


def per_device(sections, n, activations, norm_gain, in_proj, out_proj, expert_ids):
    tokens, width = activations.shape[1:]
    ff = in_proj.shape[2]
    capacity = 2 * tokens // EXPERTS
    rows = EXPERTS * capacity
    rest, back_rest, piece, half = width - FLAT, width - BACK, tokens // PIECES, RING // 2
    dma = pltpu.SemaphoreType.DMA
    vmem = pltpu.VMEM
    return pl.pallas_call(
        functools.partial(kernel, sections, n, capacity),
        out_shape=pltpu.VMEM(activations.shape, activations.dtype),
        in_specs=[pl.BlockSpec(memory_space=pl.ANY)] * 5,
        out_specs=pl.BlockSpec(memory_space=pltpu.VMEM),
        scratch_shapes=[
            vmem((tokens, width), BF16),
            vmem((1, width), F32),
            vmem((1, tokens), jnp.int32),
            vmem((width, ff), BF16),
            vmem((ff, width), BF16),
            vmem((tokens, rest), BF16),
            vmem((EXPERTS, capacity, rest), BF16),
            vmem((RING, EXPERTS, capacity, rest), BF16),
            vmem((RING, PIECES, piece, FLAT + LANES), BF16),
            vmem((RING, EXPERTS, capacity, FLAT), BF16),
            vmem((RING, EXPERTS, capacity, FLAT), BF16),
            vmem((2 * rows, ff), F32),
            vmem((2 * rows, ff), BF16),
            vmem((RING, EXPERTS, capacity, back_rest), F32),
            vmem((2 * half * EXPERTS, capacity, back_rest), BF16),
            vmem((2, half, EXPERTS, capacity, back_rest), BF16),
            vmem((EXPERTS, capacity, back_rest), BF16),
            vmem((EXPERTS, capacity, back_rest), BF16),
            vmem((RING, EXPERTS, capacity, BACK), BF16),
            vmem((RING, EXPERTS, capacity, BACK), BF16),
            vmem((RING, PIECES, piece, BACK), F32),
            vmem((2 * half * PIECES, piece, BACK), BF16),
            vmem((2, half, PIECES, piece, BACK), BF16),
            vmem((PIECES, piece, BACK), BF16),
            vmem((PIECES, piece, BACK), BF16),
            vmem((tokens, LANES), BF16),
            vmem((tokens, back_rest), BF16),
            vmem((tokens, LANES), BF16),
            dma((3,)),
            dma((2,)),
            dma((2,)),
            dma((2,)),
            dma((1,)),
            dma((1,)),
            dma((RING, EXPERTS)),
            dma((1,)),
            dma((1,)),
            dma((1,)),
            dma((1,)),
            dma((RING, PIECES)),
            dma((1,)),
            dma((RING,)),
            dma((1,)),
            dma((RING,)),
            dma((1,)),
            dma((1,)),
            dma((PIECES,)),
            pltpu.SemaphoreType.REGULAR((2,)),
        ],
        compiler_params=pltpu.CompilerParams(
            collective_id=0, has_side_effects=True, vmem_limit_bytes=62 * 1024 * 1024
        ),
    )(activations, norm_gain, expert_ids.reshape(1, tokens), in_proj, out_proj)


def solution(mesh):
    return jax.shard_map(
        functools.partial(per_device, mesh.shape["section"], mesh.shape["expert"]),
        mesh=mesh,
        in_specs=(
            P("section", "expert", None),
            P("section", None),
            P("section", None, "expert"),
            P("section", "expert", None),
            P("section", "expert", None),
        ),
        out_specs=P("section", "expert", None),
        check_vma=False,
    )
```
